128 devices in a mesh: circ: 32 (over x_hi, y, z), side: 4 (over x_lo, core).
Axes of the slice: x: 4 (x_hi: 2, x_lo: 2; x = x_hi * 2 + x_lo), y: 4, z: 4, core: 2. Of those that a mesh axis runs over, the one named last changes fastest.
Arguments:
- field: float32 [4, 7, 7, 7, 8, 4096], P('side', None, None, None, None, 'circ'), may hold values from -6 to 6
- coeffs: float32 [4, 3, 7, 7, 7, 8, 4096], P('side', None, None, None, None, None, 'circ'), may hold values from 0.25 to 1.5
- reaction: float32 [4, 7, 7, 7, 8, 4096], P('side', None, None, None, None, 'circ'), may hold values from 0.25 to 8
- step_scale: float32 [4, 7, 7, 7, 8, 4096], P('side', None, None, None, None, 'circ'), may hold values from 0.0001 to 0.0003
- rotation: int32 [4], replicated, may hold values from 0 to 12287
Outputs:
- advanced: float32 [4, 7, 7, 7, 8, 4096], P('side', None, None, None, None, 'circ')
The draws below stay inside these ranges and needn't reach their ends.
Inputs may be any that keep to these rules, and one draw needn't show every extreme that they name: `rotation`: rotor position in units of one 3-th of an element's circumferential width.
All inputs are finite; a program needn't handle non-finite values.
Results may differ from the reference program's by a relative error of at most 0.0001.
Values sent between devices are 32-bit elements; how exact they have to be, the bound alone decides.
A program may use at most 128 MiB of HBM per device.

```python
import math
import jax
import jax.numpy as jnp
import numpy as np
from jax import lax

NODES = 7
ER = 8
SUBSTEPS = 3
STEPS = 4
LAYERS = 4
NC = 4096


def plant(drawn, rng, smallest, top_value):
    dims = drawn.shape
    place = [jax.random.randint(jax.random.fold_in(rng, axis), (), 0, dims[axis]) for axis in range(len(dims))]
    drawn = drawn.at[tuple(place)].set(smallest)
    longest = dims.index(max(dims))
    place[longest] = (place[longest] + 1) % dims[longest]
    return drawn.at[tuple(place)].set(top_value)


def level_of(own_key, dims, shards, least, top_value):
    level, own = 1.0, jax.random.fold_in(own_key, 6)
    for axis_at, shards_of in shards:
        steps = jnp.exp(jax.random.uniform(jax.random.fold_in(own, axis_at), (shards_of,), jnp.float32, least / len(shards), top_value / len(shards)))
        level = level * jnp.repeat(steps, dims[axis_at] // shards_of).reshape([-1 if axis == axis_at else 1 for axis in range(len(dims))])
    return level


def noise(own_key, extent, scale, limit, pieces=(), held_as=jnp.bfloat16):
    entries = jax.random.normal(own_key, extent, jnp.float32) * scale
    if len(pieces) > 0:
        entries = level_of(own_key, extent, pieces, -0.22, 0.18) * entries
    return jnp.clip(entries, min=-limit, max=limit).astype(held_as)


def setup_inputs(seed: int = 0) -> dict:
    keys = jax.random.split(jax.random.key(seed), 6)
    field = noise(keys[0], (LAYERS, NODES, NODES, NODES, ER, NC), 1.0, 6.0, ((0, 4), (5, 32)), jnp.float32)
    coeffs = jnp.clip(jnp.exp(math.log(1.5) - 1.7917595 * jax.random.uniform(keys[1], (LAYERS, 3, NODES, NODES, NODES, ER, NC), jnp.float32) ** level_of(keys[1], (LAYERS, 3, NODES, NODES, NODES, ER, NC), ((0, 4), (6, 32)), -0.2, 0.2)), 0.25, 1.5)
    reaction = jnp.clip(jnp.exp(math.log(8.0) - 3.465736 * jax.random.uniform(keys[2], (LAYERS, NODES, NODES, NODES, ER, NC), jnp.float32) ** level_of(keys[2], (LAYERS, NODES, NODES, NODES, ER, NC), ((0, 4), (5, 32)), -0.2, 0.2)), 0.25, 8.0)
    step_scale = jnp.clip(jnp.exp(math.log(0.0003) - 1.09861236 * jax.random.uniform(keys[3], (LAYERS, NODES, NODES, NODES, ER, NC), jnp.float32) ** level_of(keys[3], (LAYERS, NODES, NODES, NODES, ER, NC), ((0, 4), (5, 32)), -0.2, 0.2)), 0.0001, 0.0003)
    rotation = plant(jax.random.randint(keys[4], (STEPS,), 0, NC * SUBSTEPS), jax.random.fold_in(keys[4], 1), 0, (NC * SUBSTEPS) - 1).astype(jnp.int32)
    return {"field": field, "coeffs": coeffs, "reaction": reaction, "step_scale": step_scale, "rotation": rotation}


def gll_points():
    return np.array([-1.0, -0.830223896278567, -0.4688487934707142, 0.0, 0.4688487934707142, 0.830223896278567, 1.0])


def derivative_table():
    points = gll_points()
    node_count = points.shape[0]
    weights = np.array([1.0 / np.prod([points[j] - points[k] for k in range(node_count) if k != j]) for j in range(node_count)])
    derivative = np.zeros((node_count, node_count))
    for i in range(node_count):
        for j in range(node_count):
            if i != j:
                derivative[i, j] = weights[j] / weights[i] / (points[i] - points[j])
        derivative[i, i] = -np.sum(derivative[i])
    return derivative


def lagrange_rows(locations):
    points = gll_points()
    identity_mask = np.eye(7) > 0.5
    differences = np.array([[1.0 if q == n else points[n] - points[q] for q in range(7)] for n in range(7)])
    denominator = np.prod(differences, axis=1)
    distances = locations[:, None] - jnp.asarray(points, jnp.float32)[None, :]
    factors = jnp.where(identity_mask[None, :, :], 1.0, distances[:, None, :])
    return jnp.prod(factors, axis=2) / jnp.asarray(denominator, jnp.float32)[None, :]


def mortar_tables(fraction):
    heights = (1.0 + jnp.asarray(gll_points(), jnp.float32)) * 0.5
    on_right = heights >= fraction
    shifted_height = jnp.where(on_right, heights - fraction, heights - fraction + 1.0)
    values = lagrange_rows(2.0 * shifted_height - 1.0)
    from_right = jnp.where(on_right[:, None], values, 0.0)
    from_left = jnp.where(on_right[:, None], 0.0, values)
    return from_left, from_right


def element_apply(field, coeffs, reaction):
    derivative = jnp.asarray(derivative_table(), jnp.float32)
    highest = lax.Precision.HIGHEST
    grad_axial = jnp.einsum("pa,arcxe->prcxe", derivative, field, precision=highest)
    grad_radial = jnp.einsum("pr,arcxe->apcxe", derivative, field, precision=highest)
    grad_circ = jnp.einsum("pc,arcxe->arpxe", derivative, field, precision=highest)
    result = reaction * field
    result = result + jnp.einsum("pa,prcxe->arcxe", derivative, coeffs[0] * grad_axial, precision=highest)
    result = result + jnp.einsum("pr,apcxe->arcxe", derivative, coeffs[1] * grad_radial, precision=highest)
    result = result + jnp.einsum("pc,arpxe->arcxe", derivative, coeffs[2] * grad_circ, precision=highest)
    return result


def layer_apply(inputs):
    return element_apply(inputs[0], inputs[1], inputs[2])


def reference(field, coeffs, reaction, step_scale, rotation):
    lower = LAYERS // 2 - 1
    highest = lax.Precision.HIGHEST
    current = field
    for step in range(STEPS):
        applied = lax.map(layer_apply, (current, coeffs, reaction))
        outer_faces = applied[:, :, 6]
        inner_faces = applied[:, :, 0]
        zero_row = jnp.zeros_like(inner_faces[:, :, :, :1])
        summed = applied.at[:, :, 6].add(jnp.concatenate([inner_faces[:, :, :, 1:], zero_row], axis=3))
        summed = summed.at[:, :, 0].add(jnp.concatenate([zero_row, outer_faces[:, :, :, :-1]], axis=3))
        summed = summed.at[:, :, :, 6].add(jnp.roll(applied[:, :, :, 0], -1, axis=4))
        summed = summed.at[:, :, :, 0].add(jnp.roll(applied[:, :, :, 6], 1, axis=4))
        top_faces = applied[:, 6]
        bottom_faces = applied[:, 0]
        offset = rotation[step]
        whole_k = (offset // SUBSTEPS).astype(jnp.int32)
        fraction = (offset % SUBSTEPS).astype(jnp.float32) / SUBSTEPS
        from_left, from_right = mortar_tables(fraction)
        rotor_top = top_faces[lower]
        stator_bottom = bottom_faces[lower + 1]
        stator_part = jnp.einsum("mn,rnxe->rmxe", from_left, jnp.roll(rotor_top, whole_k + 1, axis=3), precision=highest)
        stator_part = stator_part + jnp.einsum("mn,rnxe->rmxe", from_right, jnp.roll(rotor_top, whole_k, axis=3), precision=highest)
        rotor_part = jnp.einsum("mn,rmxe->rnxe", from_right, jnp.roll(stator_bottom, -whole_k, axis=3), precision=highest)
        rotor_part = rotor_part + jnp.einsum("mn,rmxe->rnxe", from_left, jnp.roll(stator_bottom, -whole_k - 1, axis=3), precision=highest)
        zero_face = jnp.zeros_like(top_faces[:1])
        from_below = jnp.concatenate([zero_face, top_faces[:-1]], axis=0)
        from_above = jnp.concatenate([bottom_faces[1:], zero_face], axis=0)
        from_below = from_below.at[lower + 1].set(stator_part)
        from_above = from_above.at[lower].set(rotor_part)
        summed = summed.at[:, 0].add(from_below)
        summed = summed.at[:, 6].add(from_above)
        current = current - step_scale * summed
    return current
```

```python
import jax
import jax.numpy as jnp
import numpy as np
from jax import lax
from jax.experimental import pallas as pl
from jax.experimental.pallas import tpu as pltpu
from jax.sharding import PartitionSpec as P

SUBSTEPS = 3
STEPS = 4
N = 7
NY = 4
NZ = 4
MESH = pl.DeviceIdType.MESH


def gll_points():
    return np.array(
        [-1.0, -0.830223896278567, -0.4688487934707142, 0.0,
         0.4688487934707142, 0.830223896278567, 1.0]
    )


def derivative_table():
    points = gll_points()
    weights = np.array(
        [1.0 / np.prod([points[j] - points[k] for k in range(N) if k != j]) for j in range(N)]
    )
    derivative = np.zeros((N, N))
    for i in range(N):
        for j in range(N):
            if i != j:
                derivative[i, j] = weights[j] / weights[i] / (points[i] - points[j])
        derivative[i, i] = -np.sum(derivative[i])
    return derivative


def lagrange_row(location):
    points = gll_points()
    return np.array(
        [np.prod([(location - points[q]) / (points[n] - points[q]) for q in range(N) if q != n])
         for n in range(N)]
    )


def mortar_constants():
    heights = (1.0 + gll_points()) * 0.5
    table = np.zeros((2, SUBSTEPS, 2, N, N))
    for residue in range(SUBSTEPS):
        fraction = residue / SUBSTEPS
        rows = []
        for m in range(N):
            local = heights[m] - fraction
            if heights[m] < fraction:
                local += 1.0
            rows.append(lagrange_row(2.0 * local - 1.0))
        both = np.array(rows)
        table[0, residue, 0] = both
        table[0, residue, 1] = both.T
        table[1, residue, 0] = np.eye(N)
        table[1, residue, 1] = np.eye(N)
    return table.astype(np.float32)


def left_counts():
    heights = (1.0 + gll_points()) * 0.5
    return [int(np.sum(heights < residue / SUBSTEPS)) for residue in range(SUBSTEPS)]


DERIV = derivative_table()
LEFT = left_counts()


def half_line(matrix, v):
    even = [v[q] + v[6 - q] for q in range(3)]
    odd = [v[q] - v[6 - q] for q in range(3)]
    out = [None] * N
    for p in range(3):
        e = float(matrix[p, 3]) * v[3]
        o = None
        for q in range(3):
            e = e + float(0.5 * (matrix[p, q] + matrix[p, 6 - q])) * even[q]
            term = float(0.5 * (matrix[p, q] - matrix[p, 6 - q])) * odd[q]
            o = term if o is None else o + term
        out[p] = o + e
        out[6 - p] = o - e
    out[3] = (
        float(matrix[3, 0]) * odd[0] + float(matrix[3, 1]) * odd[1] + float(matrix[3, 2]) * odd[2]
    )
    return out


def apply_line(v, coeff):
    grad = half_line(DERIV, v)
    return half_line(DERIV.T, [coeff[p] * grad[p] for p in range(N)])


def kernel(
    rot, table, field, coeffs, reaction, scale, out,
    u, co, re, sc, ap, splat, codes, face, delta, diag,
    halo_src, halo_dst, side_dst,
    zsrc, zdst, ysrc, ydst, xsrc, xdst,
    load_u, load_c, load_s, store_sem,
    halo_send, halo_recv, side_send, side_recv,
    zsend, zrecv, ysend, yrecv, xsend, xrecv,
):
    c = lax.axis_index("circ")
    side = lax.axis_index("side")
    count = lax.axis_size("circ")
    z_me = c % NZ
    y_me = (c // NZ) % NY
    x_me = c // (NZ * NY)
    is_mortar = (side == 1) | (side == 2)
    is_rotor = side < 2
    parity = side % 2
    partner = side + 1 - 2 * parity
    fp = 6 - 6 * parity
    fm = 6 * parity
    lane = lax.broadcasted_iota(jnp.int32, (8, 128), 1)
    row = lax.broadcasted_iota(jnp.int32, (8, 128), 0)

    def at(xx, yy, zz):
        return (xx * NY + yy) * NZ + zz

    nxt = (c + 1) % count
    prv = (c + count - 1) % count
    z_dev = [at(x_me, y_me, (z_me + j + 1) % NZ) for j in range(3)]
    y_dev = [at(x_me, (y_me + j + 1) % NY, z_me) for j in range(3)]
    x_dev = [at((x_me + j) % 2, y_me, z_me) for j in range(2)]
    across = 3 - side

    def load_slice(a):
        return [
            pltpu.make_async_copy(field.at[a], u.at[a], load_u.at[a, 0]),
            pltpu.make_async_copy(reaction.at[a], re.at[a], load_u.at[a, 1]),
            pltpu.make_async_copy(coeffs.at[1, a], co.at[1, a], load_u.at[a, 2]),
            pltpu.make_async_copy(coeffs.at[2, a], co.at[2, a], load_u.at[a, 3]),
        ]

    load_axial = pltpu.make_async_copy(coeffs.at[0], co.at[0], load_c)
    load_scale = pltpu.make_async_copy(scale, sc, load_s)

    barrier = pltpu.get_barrier_semaphore()

    def greet(cc, ss):
        pl.semaphore_signal(
            barrier, inc=1, device_id={"circ": cc, "side": ss}, device_id_type=MESH
        )

    greet(nxt, side)
    greet(prv, side)
    greet(c, partner)

    @pl.when(is_mortar)
    def _():
        for d in z_dev + y_dev:
            greet(d, side)
        for d in x_dev:
            greet(d, across)

    def issue(a, carry):
        for copy in load_slice(a):
            copy.start()
        return carry

    lax.fori_loop(0, N, issue, 0)
    load_axial.start()
    load_scale.start()

    def digits(shift):
        s = shift & 127
        total = ((shift >> 7) + jnp.where(lane < s, 1, 0)) & 31
        dz = total & 3
        dy = ((total >> 2) & 3) + jnp.where(z_me < dz, 1, 0)
        dx = ((total >> 4) + jnp.where(y_me < dy, 1, 0)) & 1
        return dz, dy & 3, dx

    @pl.when(is_mortar)
    def _():
        def prepare(t, carry):
            offset = rot[t]
            k = offset // SUBSTEPS
            residue = offset - k * SUBSTEPS
            left = jnp.where(residue == 0, LEFT[0], jnp.where(residue == 1, LEFT[1], LEFT[2]))
            cycle = count * 128
            for m in range(N):
                kappa = k + jnp.where(m < left, 1, 0)
                kappa = jnp.where(kappa >= cycle, kappa - cycle, kappa)
                back = jnp.where(kappa == 0, 0, cycle - kappa)
                dz, dy, _ = digits(jnp.where(is_rotor, kappa, back))
                codes[t, 0, m] = dz
                codes[t, 1, m] = dy
                codes[t, 2, m] = digits(jnp.where(is_rotor, back, kappa))[2]
            half = jnp.where(is_rotor, 0, 1)
            first = (half * SUBSTEPS + residue) * 2 * N * N
            for i in range(2 * N * N):
                splat[t, i] = jnp.full((8, 128), table[first + i], jnp.float32)
            return carry

        lax.fori_loop(0, STEPS, prepare, 0)

    def in_face(a):
        for cc in range(N):
            line = [u[a, r, cc] for r in range(N)]
            res = apply_line(line, [co[1, a, p, cc] for p in range(N)])
            for r in range(N):
                ap[a, r, cc] = res[r] + re[a, r, cc] * line[r]
        for r in range(N):
            line = [u[a, r, cc] for cc in range(N)]
            res = apply_line(line, [co[2, a, r, p] for p in range(N)])
            for cc in range(N):
                ap[a, r, cc] = ap[a, r, cc] + res[cc]

    def axial(r, carry):
        for cc in range(N):
            line = [u[a, r, cc] for a in range(N)]
            res = apply_line(line, [co[0, p, r, cc] for p in range(N)])
            for a in range(N):
                ap[a, r, cc] = ap[a, r, cc] + res[a]
        return carry

    def first_slice(a, carry):
        for copy in load_slice(a):
            copy.wait()
        in_face(a)
        return carry

    def next_slice(a, carry):
        in_face(a)
        return carry

    lax.fori_loop(0, N, first_slice, 0)
    load_axial.wait()
    lax.fori_loop(0, N, axial, 0)
    load_scale.wait()

    edge = [jnp.where(parity == 1, float(DERIV[p, 6]), float(DERIV[p, 0])) for p in range(N)]

    @pl.when(is_mortar)
    def _():
        def body(r, carry):
            for cc in range(N):
                total = re[fm, r, cc]
                for p in range(N):
                    total = total + float(DERIV[p, 0]) ** 2 * jnp.where(
                        parity == 1, co[0, 6 - p, r, cc], co[0, p, r, cc]
                    )
                diag[r, cc] = total
                face[r, cc] = ap[fm, r, cc]
            return carry

        lax.fori_loop(0, N, body, 0)

    @pl.when(is_mortar)
    def _():
        pl.semaphore_wait(barrier, 11)

    @pl.when(jnp.logical_not(is_mortar))
    def _():
        pl.semaphore_wait(barrier, 3)

    def hop(src, dst, send, recv, cc, ss):
        return pltpu.make_async_remote_copy(
            src_ref=src, dst_ref=dst, send_sem=send, recv_sem=recv,
            device_id={"circ": cc, "side": ss}, device_id_type=MESH,
        )

    def z_hop(t, r, j):
        return hop(zsrc.at[t, r], zdst.at[t, j, r], zsend.at[t, j, r], zrecv.at[t, j, r], z_dev[j], side)

    def y_hop(t, r, j):
        return hop(ysrc.at[t, r], ydst.at[t, j, r], ysend.at[t, j, r], yrecv.at[t, j, r], y_dev[j], side)

    def x_hop(t, r, j):
        return hop(xsrc.at[t, r], xdst.at[t, j, r], xsend.at[t, j, r], xrecv.at[t, j, r], x_dev[j], across)

    def step(t, carry):
        @pl.when(is_mortar)
        def _():
            offset = rot[t]
            k = offset // SUBSTEPS
            residue = offset - k * SUBSTEPS
            left = jnp.where(residue == 0, LEFT[0], jnp.where(residue == 1, LEFT[1], LEFT[2]))
            shifts = []
            for m in range(N):
                kappa = k + jnp.where(m < left, 1, 0)
                shifts.append(jnp.where(is_rotor, kappa, 128 * 64 - kappa) & 127)

            def send(r, carry):
                nodes = [face[r, n] for n in range(N)]
                for m in range(N):
                    total = splat[t, m * N] * nodes[0]
                    for n in range(1, N):
                        total = total + splat[t, m * N + n] * nodes[n]
                    zsrc[t, r, m] = pltpu.roll(total, shifts[m], 1)
                for j in range(3):
                    z_hop(t, r, j).start()
                return carry

            lax.fori_loop(0, N, send, 0)

            @pl.when(t > 0)
            def _():
                def rest(r, carry):
                    for cc in range(N):
                        d = delta[r, cc]
                        res = half_line(DERIV.T, [(edge[p] * d) * co[0, p, r, cc] for p in range(N)])
                        for a in range(N):
                            ap[a, r, cc] = ap[a, r, cc] + res[a]
                    for cc in range(N):
                        ap[fm, r, cc] = face[r, cc]
                    return carry

                lax.fori_loop(0, N, rest, 0)

        side_copy = hop(ap.at[fp], side_dst.at[t], side_send.at[t], side_recv.at[t], c, partner)
        side_copy.start()

        def pack(a, carry):
            low, high = carry
            for r in range(N):
                here = lane == a * N + r
                low = jnp.where(here, jnp.broadcast_to(ap[a, r, 0][:, 0:1], (8, 128)), low)
                high = jnp.where(here, jnp.broadcast_to(ap[a, r, 6][:, 127:128], (8, 128)), high)
            return low, high

        zero = jnp.zeros((8, 128), jnp.float32)
        low, high = lax.fori_loop(0, N, pack, (zero, zero))
        halo_src[t, 0] = low
        halo_src[t, 1] = high
        low_copy = hop(halo_src.at[t, 0], halo_dst.at[t, 0], halo_send.at[t, 0], halo_recv.at[t, 0], prv, side)
        high_copy = hop(halo_src.at[t, 1], halo_dst.at[t, 1], halo_send.at[t, 1], halo_recv.at[t, 1], nxt, side)
        low_copy.start()
        high_copy.start()
        low_copy.wait()
        high_copy.wait()

        def advance(a, carry):
            after, before = carry
            for r in range(N):
                for cc in range(N):
                    total = ap[a, r, cc]
                    if r == 6:
                        total = total + jnp.where(row == 7, 0.0, pltpu.roll(ap[a, 0, cc], 7, 0))
                    if r == 0:
                        total = total + jnp.where(row == 0, 0.0, pltpu.roll(ap[a, 6, cc], 1, 0))
                    if cc == 6:
                        other = jnp.broadcast_to(after[:, r:r + 1], (8, 128))
                        total = total + jnp.where(lane == 127, other, pltpu.roll(ap[a, r, 0], 127, 1))
                    if cc == 0:
                        other = jnp.broadcast_to(before[:, r:r + 1], (8, 128))
                        total = total + jnp.where(lane == 0, other, pltpu.roll(ap[a, r, 6], 1, 1))
                    u[a, r, cc] = u[a, r, cc] - sc[a, r, cc] * total
            return pltpu.roll(after, 128 - N, 1), pltpu.roll(before, 128 - N, 1)

        lax.fori_loop(0, N, advance, (halo_dst[t, 0], halo_dst[t, 1]))
        side_copy.wait()

        def add_side(r, carry):
            for cc in range(N):
                u[fp, r, cc] = u[fp, r, cc] - sc[fp, r, cc] * side_dst[t, r, cc]
            return carry

        lax.fori_loop(0, N, add_side, 0)

        @pl.when(is_mortar)
        def _():
            def along_y(r, carry):
                for j in range(3):
                    z_hop(t, r, j).wait_recv()
                for m in range(N):
                    code = codes[t, 0, m]
                    low = jnp.where(code == 0, zsrc[t, r, m], zdst[t, 0, r, m])
                    high = jnp.where(code == 2, zdst[t, 1, r, m], zdst[t, 2, r, m])
                    ysrc[t, r, m] = jnp.where(code < 2, low, high)
                for j in range(3):
                    y_hop(t, r, j).start()
                return carry

            lax.fori_loop(0, N, along_y, 0)

            def along_x(r, carry):
                for j in range(3):
                    y_hop(t, r, j).wait_recv()
                for m in range(N):
                    code = codes[t, 1, m]
                    low = jnp.where(code == 0, ysrc[t, r, m], ydst[t, 0, r, m])
                    high = jnp.where(code == 2, ydst[t, 1, r, m], ydst[t, 2, r, m])
                    xsrc[t, r, m] = jnp.where(code < 2, low, high)
                for j in range(2):
                    x_hop(t, r, j).start()
                return carry

            lax.fori_loop(0, N, along_x, 0)

        @pl.when(t < STEPS - 1)
        def _():
            lax.fori_loop(0, N, next_slice, 0)
            lax.fori_loop(0, N, axial, 0)

        @pl.when(is_mortar)
        def _():
            def arrive(r, carry):
                for j in range(2):
                    x_hop(t, r, j).wait_recv()
                nodes = [
                    jnp.where(codes[t, 2, m] == 0, xdst[t, 0, r, m], xdst[t, 1, r, m])
                    for m in range(N)
                ]
                for n in range(N):
                    total = splat[t, N * N + n * N] * nodes[0]
                    for m in range(1, N):
                        total = total + splat[t, N * N + n * N + m] * nodes[m]
                    change = -(sc[fm, r, n] * total)
                    delta[r, n] = change
                    u[fm, r, n] = u[fm, r, n] + change
                return carry

            lax.fori_loop(0, N, arrive, 0)

            @pl.when(t < STEPS - 1)
            def _():
                for cc in range(N):
                    line = [delta[r, cc] for r in range(N)]
                    res = apply_line(line, [co[1, fm, p, cc] for p in range(N)])
                    for r in range(N):
                        face[r, cc] = ap[fm, r, cc] + res[r] + diag[r, cc] * line[r]
                for r in range(N):
                    line = [delta[r, cc] for cc in range(N)]
                    res = apply_line(line, [co[2, fm, r, p] for p in range(N)])
                    for cc in range(N):
                        face[r, cc] = face[r, cc] + res[cc]

            def drain(r, carry):
                for j in range(3):
                    z_hop(t, r, j).wait_send()
                    y_hop(t, r, j).wait_send()
                for j in range(2):
                    x_hop(t, r, j).wait_send()
                return carry

            lax.fori_loop(0, N, drain, 0)

        return carry

    lax.fori_loop(0, STEPS, step, 0)
    done = pltpu.make_async_copy(u, out, store_sem)
    done.start()
    done.wait()


def local(field, coeffs, reaction, step_scale, rotation):
    block = field.shape[1:]
    tile = block[-2:]
    f32 = jnp.float32
    dma = pltpu.SemaphoreType.DMA
    table = jnp.asarray(mortar_constants().reshape(-1))
    any_spec = pl.BlockSpec(memory_space=pl.ANY)
    smem_spec = pl.BlockSpec(memory_space=pltpu.SMEM)

    def face_buffers(*lead):
        return pltpu.VMEM((*lead, N, N, *tile), f32)

    result = pl.pallas_call(
        kernel,
        out_shape=jax.ShapeDtypeStruct(block, f32),
        in_specs=[smem_spec, smem_spec, any_spec, any_spec, any_spec, any_spec],
        out_specs=any_spec,
        scratch_shapes=[
            pltpu.VMEM(block, f32),
            pltpu.VMEM((3, *block), f32),
            pltpu.VMEM(block, f32),
            pltpu.VMEM(block, f32),
            pltpu.VMEM(block, f32),
            pltpu.VMEM((STEPS, 2 * N * N, *tile), f32),
            pltpu.VMEM((STEPS, 3, N, *tile), jnp.int32),
            face_buffers(),
            face_buffers(),
            face_buffers(),
            pltpu.VMEM((STEPS, 2, *tile), f32),
            pltpu.VMEM((STEPS, 2, *tile), f32),
            face_buffers(STEPS),
            face_buffers(STEPS),
            face_buffers(STEPS, 3),
            face_buffers(STEPS),
            face_buffers(STEPS, 3),
            face_buffers(STEPS),
            face_buffers(STEPS, 2),
            dma((N, 4)),
            dma,
            dma,
            dma,
            dma((STEPS, 2)),
            dma((STEPS, 2)),
            dma((STEPS,)),
            dma((STEPS,)),
            dma((STEPS, 3, N)),
            dma((STEPS, 3, N)),
            dma((STEPS, 3, N)),
            dma((STEPS, 3, N)),
            dma((STEPS, 2, N)),
            dma((STEPS, 2, N)),
        ],
        compiler_params=pltpu.CompilerParams(
            collective_id=0, has_side_effects=True, vmem_limit_bytes=60 * 1024 * 1024
        ),
    )(rotation, table, field[0], coeffs[0], reaction[0], step_scale[0])
    return result[None]


def solution(mesh):
    in_specs = (
        P("side", None, None, None, None, "circ"),
        P("side", None, None, None, None, None, "circ"),
        P("side", None, None, None, None, "circ"),
        P("side", None, None, None, None, "circ"),
        P(),
    )
    out_specs = P("side", None, None, None, None, "circ")
    return jax.shard_map(local, mesh=mesh, in_specs=in_specs, out_specs=out_specs, check_vma=False)
```

```python
import jax
import jax.numpy as jnp
import numpy as np
from jax import lax
from jax.experimental import pallas as pl
from jax.experimental.pallas import tpu as pltpu
from jax.sharding import PartitionSpec as P

SUBSTEPS = 3
STEPS = 4
N = 7
NY = 4
NZ = 4
SPLIT = 4
MESH = pl.DeviceIdType.MESH


def gll_points():
    return np.array(
        [-1.0, -0.830223896278567, -0.4688487934707142, 0.0,
         0.4688487934707142, 0.830223896278567, 1.0]
    )


def derivative_table():
    points = gll_points()
    weights = np.array(
        [1.0 / np.prod([points[j] - points[k] for k in range(N) if k != j]) for j in range(N)]
    )
    derivative = np.zeros((N, N))
    for i in range(N):
        for j in range(N):
            if i != j:
                derivative[i, j] = weights[j] / weights[i] / (points[i] - points[j])
        derivative[i, i] = -np.sum(derivative[i])
    return derivative


def lagrange_row(location):
    points = gll_points()
    return np.array(
        [np.prod([(location - points[q]) / (points[n] - points[q]) for q in range(N) if q != n])
         for n in range(N)]
    )


def mortar_constants():
    heights = (1.0 + gll_points()) * 0.5
    table = np.zeros((2, SUBSTEPS, 2, N, N))
    for residue in range(SUBSTEPS):
        fraction = residue / SUBSTEPS
        rows = []
        for m in range(N):
            local = heights[m] - fraction
            if heights[m] < fraction:
                local += 1.0
            rows.append(lagrange_row(2.0 * local - 1.0))
        both = np.array(rows)
        table[0, residue, 0] = both
        table[0, residue, 1] = both.T
        table[1, residue, 0] = np.eye(N)
        table[1, residue, 1] = np.eye(N)
    return table.astype(np.float32)


def left_counts():
    heights = (1.0 + gll_points()) * 0.5
    return [int(np.sum(heights < residue / SUBSTEPS)) for residue in range(SUBSTEPS)]


DERIV = derivative_table()
LEFT = left_counts()


def half_line(matrix, v):
    even = [v[q] + v[6 - q] for q in range(3)]
    odd = [v[q] - v[6 - q] for q in range(3)]
    out = [None] * N
    for p in range(3):
        e = float(matrix[p, 3]) * v[3]
        o = None
        for q in range(3):
            e = e + float(0.5 * (matrix[p, q] + matrix[p, 6 - q])) * even[q]
            term = float(0.5 * (matrix[p, q] - matrix[p, 6 - q])) * odd[q]
            o = term if o is None else o + term
        out[p] = o + e
        out[6 - p] = o - e
    out[3] = (
        float(matrix[3, 0]) * odd[0] + float(matrix[3, 1]) * odd[1] + float(matrix[3, 2]) * odd[2]
    )
    return out


def apply_line(v, coeff):
    grad = half_line(DERIV, v)
    return half_line(DERIV.T, [coeff[p] * grad[p] for p in range(N)])


def kernel(
    rot, table, field, coeffs, reaction, scale, u,
    co, re, sc, ap, splat, codes, face, delta, diag,
    halo_src, halo_dst, side_dst,
    src1, dst1, src2, dst2, src3, dst3,
    load_u, load_c, load_s,
    halo_send, halo_recv, side_send, side_recv,
    send1, recv1, send2, recv2, send3, recv3,
):
    c = lax.axis_index("circ")
    side = lax.axis_index("side")
    count = lax.axis_size("circ")
    z_me = c % NZ
    y_me = (c // NZ) % NY
    x_me = c // (NZ * NY)
    is_mortar = (side == 1) | (side == 2)
    is_rotor = side < 2
    parity = side % 2
    partner = side + 1 - 2 * parity
    fp = 6 - 6 * parity
    fm = 6 * parity
    lane = lax.broadcasted_iota(jnp.int32, (8, 128), 1)
    row = lax.broadcasted_iota(jnp.int32, (8, 128), 0)

    def at(xx, yy, zz):
        return (xx * NY + yy) * NZ + zz

    nxt = (c + 1) % count
    prv = (c + count - 1) % count
    z_dev = [at(x_me, y_me, (z_me + j + 1) % NZ) for j in range(3)]
    y_dev = [at(x_me, (y_me + j + 1) % NY, z_me) for j in range(3)]
    x_dev = [at((x_me + j) % 2, y_me, z_me) for j in range(2)]
    across = 3 - side

    def ordered(i):
        return jnp.where(parity == 1, 6 - i, i)

    def load_slice(a):
        return [
            pltpu.make_async_copy(reaction.at[a], re.at[a], load_u.at[a, 0]),
            pltpu.make_async_copy(coeffs.at[1, a], co.at[1, a], load_u.at[a, 1]),
            pltpu.make_async_copy(coeffs.at[2, a], co.at[2, a], load_u.at[a, 2]),
        ]

    load_field = pltpu.make_async_copy(field, u, load_c.at[0])
    load_axial = pltpu.make_async_copy(coeffs.at[0], co.at[0], load_c.at[1])
    load_scale = pltpu.make_async_copy(scale, sc, load_s)

    barrier = pltpu.get_barrier_semaphore()

    def greet(cc, ss):
        pl.semaphore_signal(
            barrier, inc=1, device_id={"circ": cc, "side": ss}, device_id_type=MESH
        )

    greet(nxt, side)
    greet(prv, side)
    greet(c, partner)

    @pl.when(is_mortar)
    def _():
        for d in z_dev + y_dev:
            greet(d, side)
        for d in x_dev:
            greet(d, across)

    load_field.start()
    for copy in load_slice(fm):
        copy.start()
    load_axial.start()

    def issue(i, carry):
        for copy in load_slice(ordered(i)):
            copy.start()
        return carry

    lax.fori_loop(1, N, issue, 0)
    load_scale.start()

    def digits(shift):
        s = shift & 127
        total = ((shift >> 7) + jnp.where(lane < s, 1, 0)) & 31
        dz = total & 3
        dy = (total >> 2) & 3
        late = dy + jnp.where(z_me < dz, 1, 0)
        early = dy + jnp.where(z_me + dz > 3, 1, 0)
        dx = ((total >> 4) + jnp.where(y_me < late, 1, 0)) & 1
        return dz, early & 3, late & 3, dx

    @pl.when(is_mortar)
    def _():
        def prepare(t, carry):
            offset = rot[t]
            k = offset // SUBSTEPS
            residue = offset - k * SUBSTEPS
            left = jnp.where(residue == 0, LEFT[0], jnp.where(residue == 1, LEFT[1], LEFT[2]))
            cycle = count * 128
            for m in range(N):
                kappa = k + jnp.where(m < left, 1, 0)
                kappa = jnp.where(kappa >= cycle, kappa - cycle, kappa)
                back = jnp.where(kappa == 0, 0, cycle - kappa)
                dz, early, late, _ = digits(jnp.where(is_rotor, kappa, back))
                codes[t, 0, m] = dz
                codes[t, 1, m] = early
                codes[t, 2, m] = late
                codes[t, 3, m] = digits(jnp.where(is_rotor, back, kappa))[3]
            half = jnp.where(is_rotor, 0, 1)
            first = (half * SUBSTEPS + residue) * 2 * N * N
            for i in range(2 * N * N):
                splat[t, i] = jnp.full((8, 128), table[first + i], jnp.float32)
            return carry

        lax.fori_loop(0, STEPS, prepare, 0)

    def in_face(a):
        for cc in range(N):
            line = [u[a, r, cc] for r in range(N)]
            res = apply_line(line, [co[1, a, p, cc] for p in range(N)])
            for r in range(N):
                ap[a, r, cc] = res[r] + re[a, r, cc] * line[r]
        for r in range(N):
            line = [u[a, r, cc] for cc in range(N)]
            res = apply_line(line, [co[2, a, r, p] for p in range(N)])
            for cc in range(N):
                ap[a, r, cc] = ap[a, r, cc] + res[cc]

    def axial(r, carry):
        for cc in range(N):
            line = [u[a, r, cc] for a in range(N)]
            res = apply_line(line, [co[0, p, r, cc] for p in range(N)])
            for a in range(N):
                ap[a, r, cc] = ap[a, r, cc] + res[a]
        return carry

    def next_slice(a, carry):
        in_face(a)
        return carry

    edge = [jnp.where(parity == 1, float(DERIV[p, 6]), float(DERIV[p, 0])) for p in range(N)]

    load_field.wait()
    for copy in load_slice(fm):
        copy.wait()
    in_face(fm)
    load_axial.wait()

    @pl.when(is_mortar)
    def _():
        def body(r, carry):
            for cc in range(N):
                grad = half_line(DERIV, [u[a, r, cc] for a in range(N)])
                total = ap[fm, r, cc]
                for p in range(N):
                    total = total + edge[p] * (co[0, p, r, cc] * grad[p])
                face[r, cc] = total
            return carry

        lax.fori_loop(0, N, body, 0)

    @pl.when(is_mortar)
    def _():
        pl.semaphore_wait(barrier, 11)

    @pl.when(jnp.logical_not(is_mortar))
    def _():
        pl.semaphore_wait(barrier, 3)

    def hop(src, dst, send, recv, cc, ss):
        return pltpu.make_async_remote_copy(
            src_ref=src, dst_ref=dst, send_sem=send, recv_sem=recv,
            device_id={"circ": cc, "side": ss}, device_id_type=MESH,
        )

    def mixed(i):
        return i // 2 + SPLIT * (i % 2)

    def first_hop(t, r, j):
        dev = jnp.where(r < SPLIT, z_dev[j], y_dev[j])
        return hop(src1.at[t, r], dst1.at[t, j, r], send1.at[t, j, r], recv1.at[t, j, r], dev, side)

    def second_hop(t, r, j):
        dev = jnp.where(r < SPLIT, y_dev[j], z_dev[j])
        return hop(src2.at[t, r], dst2.at[t, j, r], send2.at[t, j, r], recv2.at[t, j, r], dev, side)

    def last_hop(t, r, j):
        return hop(src3.at[t, r], dst3.at[t, j, r], send3.at[t, j, r], recv3.at[t, j, r], x_dev[j], across)

    def pick(code, own, others):
        low = jnp.where(code == 0, own, others[0])
        high = jnp.where(code == 2, others[1], others[2])
        return jnp.where(code < 2, low, high)

    def step(t, carry):
        @pl.when(is_mortar)
        def _():
            offset = rot[t]
            k = offset // SUBSTEPS
            residue = offset - k * SUBSTEPS
            left = jnp.where(residue == 0, LEFT[0], jnp.where(residue == 1, LEFT[1], LEFT[2]))
            shifts = []
            for m in range(N):
                kappa = k + jnp.where(m < left, 1, 0)
                shifts.append(jnp.where(is_rotor, kappa, 128 * 64 - kappa) & 127)

            def send(i, carry):
                r = mixed(i)
                nodes = [face[r, n] for n in range(N)]
                for m in range(N):
                    total = splat[t, m * N] * nodes[0]
                    for n in range(1, N):
                        total = total + splat[t, m * N + n] * nodes[n]
                    src1[t, r, m] = pltpu.roll(total, shifts[m], 1)
                for j in range(3):
                    first_hop(t, r, j).start()
                return carry

            lax.fori_loop(0, N, send, 0)

            @pl.when(t > 0)
            def _():
                def rest(r, carry):
                    for cc in range(N):
                        d = delta[r, cc]
                        res = half_line(DERIV.T, [(edge[p] * d) * co[0, p, r, cc] for p in range(N)])
                        for a in range(N):
                            ap[a, r, cc] = ap[a, r, cc] + res[a]
                    for cc in range(N):
                        ap[fm, r, cc] = face[r, cc]
                    return carry

                lax.fori_loop(0, N, rest, 0)

        @pl.when(t == 0)
        def _():
            def first_slice(i, carry):
                a = ordered(i)
                for copy in load_slice(a):
                    copy.wait()
                in_face(a)
                return carry

            lax.fori_loop(1, N, first_slice, 0)
            lax.fori_loop(0, N, axial, 0)
            load_scale.wait()

            @pl.when(is_mortar)
            def _():
                def body(r, carry):
                    for cc in range(N):
                        total = re[fm, r, cc]
                        for p in range(N):
                            total = total + float(DERIV[p, 0]) ** 2 * jnp.where(
                                parity == 1, co[0, 6 - p, r, cc], co[0, p, r, cc]
                            )
                        diag[r, cc] = total
                    return carry

                lax.fori_loop(0, N, body, 0)

        side_copy = hop(ap.at[fp], side_dst.at[t], side_send.at[t], side_recv.at[t], c, partner)
        side_copy.start()

        def pack(a, carry):
            low, high = carry
            for r in range(N):
                here = lane == a * N + r
                low = jnp.where(here, jnp.broadcast_to(ap[a, r, 0][:, 0:1], (8, 128)), low)
                high = jnp.where(here, jnp.broadcast_to(ap[a, r, 6][:, 127:128], (8, 128)), high)
            return low, high

        zero = jnp.zeros((8, 128), jnp.float32)
        low, high = lax.fori_loop(0, N, pack, (zero, zero))
        halo_src[t, 0] = low
        halo_src[t, 1] = high
        low_copy = hop(halo_src.at[t, 0], halo_dst.at[t, 0], halo_send.at[t, 0], halo_recv.at[t, 0], prv, side)
        high_copy = hop(halo_src.at[t, 1], halo_dst.at[t, 1], halo_send.at[t, 1], halo_recv.at[t, 1], nxt, side)
        low_copy.start()
        high_copy.start()

        @pl.when(is_mortar)
        def _():
            def first_relay(i, carry):
                r = mixed(i)
                for j in range(3):
                    first_hop(t, r, j).wait_recv()
                which = jnp.where(r < SPLIT, 0, 1)
                for m in range(N):
                    src2[t, r, m] = pick(
                        codes[t, which, m], src1[t, r, m], [dst1[t, j, r, m] for j in range(3)]
                    )
                for j in range(3):
                    second_hop(t, r, j).start()
                return carry

            lax.fori_loop(0, N, first_relay, 0)

        low_copy.wait()
        high_copy.wait()

        def advance(a, carry):
            after, before = carry
            for r in range(N):
                for cc in range(N):
                    total = ap[a, r, cc]
                    if r == 6:
                        total = total + jnp.where(row == 7, 0.0, pltpu.roll(ap[a, 0, cc], 7, 0))
                    if r == 0:
                        total = total + jnp.where(row == 0, 0.0, pltpu.roll(ap[a, 6, cc], 1, 0))
                    if cc == 6:
                        other = jnp.broadcast_to(after[:, r:r + 1], (8, 128))
                        total = total + jnp.where(lane == 127, other, pltpu.roll(ap[a, r, 0], 127, 1))
                    if cc == 0:
                        other = jnp.broadcast_to(before[:, r:r + 1], (8, 128))
                        total = total + jnp.where(lane == 0, other, pltpu.roll(ap[a, r, 6], 1, 1))
                    u[a, r, cc] = u[a, r, cc] - sc[a, r, cc] * total
            return pltpu.roll(after, 128 - N, 1), pltpu.roll(before, 128 - N, 1)

        lax.fori_loop(0, N, advance, (halo_dst[t, 0], halo_dst[t, 1]))
        side_copy.wait()

        def add_side(r, carry):
            for cc in range(N):
                u[fp, r, cc] = u[fp, r, cc] - sc[fp, r, cc] * side_dst[t, r, cc]
            return carry

        lax.fori_loop(0, N, add_side, 0)

        def relay(i, carry):
            @pl.when(is_mortar)
            def _():
                r = mixed(i)
                for j in range(3):
                    second_hop(t, r, j).wait_recv()
                which = jnp.where(r < SPLIT, 2, 0)
                for m in range(N):
                    src3[t, r, m] = pick(
                        codes[t, which, m], src2[t, r, m], [dst2[t, j, r, m] for j in range(3)]
                    )
                for j in range(2):
                    last_hop(t, r, j).start()

            @pl.when(t < STEPS - 1)
            def _():
                in_face(i)

            return carry

        lax.fori_loop(0, N, relay, 0)

        @pl.when(t < STEPS - 1)
        def _():
            lax.fori_loop(0, N, axial, 0)

        @pl.when(is_mortar)
        def _():
            def arrive(i, carry):
                r = mixed(i)
                for j in range(2):
                    last_hop(t, r, j).wait_recv()
                nodes = [
                    jnp.where(codes[t, 3, m] == 0, dst3[t, 0, r, m], dst3[t, 1, r, m])
                    for m in range(N)
                ]
                for n in range(N):
                    total = splat[t, N * N + n * N] * nodes[0]
                    for m in range(1, N):
                        total = total + splat[t, N * N + n * N + m] * nodes[m]
                    change = -(sc[fm, r, n] * total)
                    delta[r, n] = change
                    u[fm, r, n] = u[fm, r, n] + change
                return carry

            lax.fori_loop(0, N, arrive, 0)

            @pl.when(t < STEPS - 1)
            def _():
                for cc in range(N):
                    line = [delta[r, cc] for r in range(N)]
                    res = apply_line(line, [co[1, fm, p, cc] for p in range(N)])
                    for r in range(N):
                        face[r, cc] = ap[fm, r, cc] + res[r] + diag[r, cc] * line[r]
                for r in range(N):
                    line = [delta[r, cc] for cc in range(N)]
                    res = apply_line(line, [co[2, fm, r, p] for p in range(N)])
                    for cc in range(N):
                        face[r, cc] = face[r, cc] + res[cc]

            def drain(r, carry):
                for j in range(3):
                    first_hop(t, r, j).wait_send()
                    second_hop(t, r, j).wait_send()
                for j in range(2):
                    last_hop(t, r, j).wait_send()
                return carry

            lax.fori_loop(0, N, drain, 0)

        return carry

    lax.fori_loop(0, STEPS, step, 0)


def local(field, coeffs, reaction, step_scale, rotation):
    block = field.shape[1:]
    tile = block[-2:]
    f32 = jnp.float32
    dma = pltpu.SemaphoreType.DMA
    table = jnp.asarray(mortar_constants().reshape(-1))
    hbm_spec = pl.BlockSpec(memory_space=pltpu.HBM)
    smem_spec = pl.BlockSpec(memory_space=pltpu.SMEM)

    def face_buffers(*lead):
        return pltpu.VMEM((*lead, N, N, *tile), f32)

    result = pl.pallas_call(
        kernel,
        out_shape=pltpu.VMEM(block, f32),
        in_specs=[smem_spec, smem_spec, hbm_spec, hbm_spec, hbm_spec, hbm_spec],
        out_specs=pl.BlockSpec(memory_space=pltpu.VMEM),
        scratch_shapes=[
            pltpu.VMEM((3, *block), f32),
            pltpu.VMEM(block, f32),
            pltpu.VMEM(block, f32),
            pltpu.VMEM(block, f32),
            pltpu.VMEM((STEPS, 2 * N * N, *tile), f32),
            pltpu.VMEM((STEPS, 4, N, *tile), jnp.int32),
            face_buffers(),
            face_buffers(),
            face_buffers(),
            pltpu.VMEM((STEPS, 2, *tile), f32),
            pltpu.VMEM((STEPS, 2, *tile), f32),
            face_buffers(STEPS),
            face_buffers(STEPS),
            face_buffers(STEPS, 3),
            face_buffers(STEPS),
            face_buffers(STEPS, 3),
            face_buffers(STEPS),
            face_buffers(STEPS, 2),
            dma((N, 3)),
            dma((2,)),
            dma,
            dma((STEPS, 2)),
            dma((STEPS, 2)),
            dma((STEPS,)),
            dma((STEPS,)),
            dma((STEPS, 3, N)),
            dma((STEPS, 3, N)),
            dma((STEPS, 3, N)),
            dma((STEPS, 3, N)),
            dma((STEPS, 2, N)),
            dma((STEPS, 2, N)),
        ],
        compiler_params=pltpu.CompilerParams(
            collective_id=0, has_side_effects=True, vmem_limit_bytes=61 * 1024 * 1024
        ),
    )(rotation, table, field[0], coeffs[0], reaction[0], step_scale[0])
    return result[None]


def solution(mesh):
    in_specs = (
        P("side", None, None, None, None, "circ"),
        P("side", None, None, None, None, None, "circ"),
        P("side", None, None, None, None, "circ"),
        P("side", None, None, None, None, "circ"),
        P(),
    )
    out_specs = P("side", None, None, None, None, "circ")
    return jax.shard_map(local, mesh=mesh, in_specs=in_specs, out_specs=out_specs, check_vma=False)
```

```python
import jax
import jax.numpy as jnp
import numpy as np
from jax import lax
from jax.experimental import pallas as pl
from jax.experimental.pallas import tpu as pltpu
from jax.sharding import PartitionSpec as P

SUBSTEPS = 3
STEPS = 4
N = 7
NY = 4
NZ = 4
PIECES = ((0, 4), (4, 3))
MESH = pl.DeviceIdType.MESH


def gll_points():
    return np.array(
        [-1.0, -0.830223896278567, -0.4688487934707142, 0.0,
         0.4688487934707142, 0.830223896278567, 1.0]
    )


def derivative_table():
    points = gll_points()
    weights = np.array(
        [1.0 / np.prod([points[j] - points[k] for k in range(N) if k != j]) for j in range(N)]
    )
    derivative = np.zeros((N, N))
    for i in range(N):
        for j in range(N):
            if i != j:
                derivative[i, j] = weights[j] / weights[i] / (points[i] - points[j])
        derivative[i, i] = -np.sum(derivative[i])
    return derivative


def lagrange_row(location):
    points = gll_points()
    return np.array(
        [np.prod([(location - points[q]) / (points[n] - points[q]) for q in range(N) if q != n])
         for n in range(N)]
    )


def mortar_constants():
    heights = (1.0 + gll_points()) * 0.5
    table = np.zeros((2, SUBSTEPS, 2, N, N))
    for residue in range(SUBSTEPS):
        fraction = residue / SUBSTEPS
        rows = []
        for m in range(N):
            local = heights[m] - fraction
            if heights[m] < fraction:
                local += 1.0
            rows.append(lagrange_row(2.0 * local - 1.0))
        both = np.array(rows)
        table[0, residue, 0] = both
        table[0, residue, 1] = both.T
        table[1, residue, 0] = np.eye(N)
        table[1, residue, 1] = np.eye(N)
    return table.astype(np.float32)


def left_counts():
    heights = (1.0 + gll_points()) * 0.5
    return [int(np.sum(heights < residue / SUBSTEPS)) for residue in range(SUBSTEPS)]


DERIV = derivative_table()
LEFT = left_counts()


def half_line(matrix, v):
    even = [v[q] + v[6 - q] for q in range(3)]
    odd = [v[q] - v[6 - q] for q in range(3)]
    out = [None] * N
    for p in range(3):
        e = float(matrix[p, 3]) * v[3]
        o = None
        for q in range(3):
            e = e + float(0.5 * (matrix[p, q] + matrix[p, 6 - q])) * even[q]
            term = float(0.5 * (matrix[p, q] - matrix[p, 6 - q])) * odd[q]
            o = term if o is None else o + term
        out[p] = o + e
        out[6 - p] = o - e
    out[3] = (
        float(matrix[3, 0]) * odd[0] + float(matrix[3, 1]) * odd[1] + float(matrix[3, 2]) * odd[2]
    )
    return out


def apply_line(v, coeff):
    grad = half_line(DERIV, v)
    return half_line(DERIV.T, [coeff[p] * grad[p] for p in range(N)])


def kernel(
    rot, table, field, coeffs, reaction, scale, u,
    co, re, sc, ap, splat, codes, face, delta, diag,
    halo_src, halo_dst, side_dst,
    src1, dst1, src2, dst2, src3, dst3,
    load_u, load_c, load_s,
    halo_send, halo_recv, side_send, side_recv,
    send0, recv0, send1, recv1, send2, recv2, send3, recv3,
):
    c = lax.axis_index("circ")
    side = lax.axis_index("side")
    count = lax.axis_size("circ")
    z_me = c % NZ
    y_me = (c // NZ) % NY
    x_me = c // (NZ * NY)
    parity = side % 2
    is_mortar = (side == 1) | (side == 2)
    is_relay = parity == 1
    is_rotor = side < 2
    partner = side + 1 - 2 * parity
    fp = 6 - 6 * parity
    fm = 6 * parity
    lane = lax.broadcasted_iota(jnp.int32, (8, 128), 1)
    row = lax.broadcasted_iota(jnp.int32, (8, 128), 0)

    def at(xx, yy, zz):
        return (xx * NY + yy) * NZ + zz

    nxt = (c + 1) % count
    prv = (c + count - 1) % count
    z_dev = [at(x_me, y_me, (z_me + j + 1) % NZ) for j in range(3)]
    y_dev = [at(x_me, (y_me + j + 1) % NY, z_me) for j in range(3)]
    x_dev = [at((x_me + j) % 2, y_me, z_me) for j in range(2)]
    first_side = jnp.where(side == 1, 1, 3)
    last_side = jnp.where(side == 1, 2, 1)

    def ordered(i):
        return jnp.where(parity == 1, 6 - i, i)

    def load_slice(a):
        return [
            pltpu.make_async_copy(reaction.at[a], re.at[a], load_u.at[a, 0]),
            pltpu.make_async_copy(coeffs.at[1, a], co.at[1, a], load_u.at[a, 1]),
            pltpu.make_async_copy(coeffs.at[2, a], co.at[2, a], load_u.at[a, 2]),
        ]

    load_field = pltpu.make_async_copy(field, u, load_c.at[0])
    load_axial = pltpu.make_async_copy(coeffs.at[0], co.at[0], load_c.at[1])
    load_scale = pltpu.make_async_copy(scale, sc, load_s)

    barrier = pltpu.get_barrier_semaphore()

    def greet(cc, ss):
        pl.semaphore_signal(
            barrier, inc=1, device_id={"circ": cc, "side": ss}, device_id_type=MESH
        )

    greet(nxt, side)
    greet(prv, side)
    greet(c, partner)

    ring = z_dev + y_dev
    peers = {
        1: [(d, 1) for d in ring] + [(d, 2) for d in x_dev] + [(d, 3) for d in x_dev],
        2: [(d, 3) for d in ring] + [(d, 1) for d in x_dev],
        3: [(d, 2) for d in ring] + [(d, 3) for d in ring] + [(d, 1) for d in x_dev],
    }

    def greet_peers(which):
        @pl.when(side == which)
        def _():
            for d, ss in peers[which]:
                greet(d, ss)

    for which in peers:
        greet_peers(which)

    load_field.start()
    for copy in load_slice(fm):
        copy.start()
    load_axial.start()

    def issue(i, carry):
        for copy in load_slice(ordered(i)):
            copy.start()
        return carry

    lax.fori_loop(1, N, issue, 0)
    load_scale.start()

    def digits(shift):
        s = shift & 127
        total = ((shift >> 7) + jnp.where(lane < s, 1, 0)) & 31
        dz = total & 3
        dy = (total >> 2) & 3
        late = dy + jnp.where(z_me < dz, 1, 0)
        early = dy + jnp.where(z_me + dz > 3, 1, 0)
        dx = ((total >> 4) + jnp.where(y_me < late, 1, 0)) & 1
        return dz, early & 3, late & 3, dx

    @pl.when(side > 0)
    def _():
        def prepare(t, carry):
            offset = rot[t]
            k = offset // SUBSTEPS
            residue = offset - k * SUBSTEPS
            left = jnp.where(residue == 0, LEFT[0], jnp.where(residue == 1, LEFT[1], LEFT[2]))
            cycle = count * 128
            for m in range(N):
                kappa = k + jnp.where(m < left, 1, 0)
                kappa = jnp.where(kappa >= cycle, kappa - cycle, kappa)
                back = jnp.where(kappa == 0, 0, cycle - kappa)
                dz, early, late, _ = digits(jnp.where(is_rotor, kappa, back))
                codes[t, 0, m] = dz
                codes[t, 1, m] = early
                codes[t, 2, m] = late
                codes[t, 3, m] = digits(jnp.where(is_rotor, back, kappa))[3]
            half = jnp.where(is_rotor, 0, 1)
            first = (half * SUBSTEPS + residue) * 2 * N * N
            for i in range(2 * N * N):
                splat[t, i] = jnp.full((8, 128), table[first + i], jnp.float32)
            return carry

        lax.fori_loop(0, STEPS, prepare, 0)

    def in_face(a):
        for cc in range(N):
            line = [u[a, r, cc] for r in range(N)]
            res = apply_line(line, [co[1, a, p, cc] for p in range(N)])
            for r in range(N):
                ap[a, r, cc] = res[r] + re[a, r, cc] * line[r]
        for r in range(N):
            line = [u[a, r, cc] for cc in range(N)]
            res = apply_line(line, [co[2, a, r, p] for p in range(N)])
            for cc in range(N):
                ap[a, r, cc] = ap[a, r, cc] + res[cc]

    def axial(r, carry):
        for cc in range(N):
            line = [u[a, r, cc] for a in range(N)]
            res = apply_line(line, [co[0, p, r, cc] for p in range(N)])
            for a in range(N):
                ap[a, r, cc] = ap[a, r, cc] + res[a]
        return carry

    def next_slice(a, carry):
        in_face(a)
        return carry

    edge = [jnp.where(parity == 1, float(DERIV[p, 6]), float(DERIV[p, 0])) for p in range(N)]

    load_field.wait()
    for copy in load_slice(fm):
        copy.wait()
    in_face(fm)
    load_axial.wait()

    @pl.when(is_mortar)
    def _():
        def body(r, carry):
            for cc in range(N):
                grad = half_line(DERIV, [u[a, r, cc] for a in range(N)])
                total = ap[fm, r, cc]
                for p in range(N):
                    total = total + edge[p] * (co[0, p, r, cc] * grad[p])
                face[r, cc] = total
            return carry

        lax.fori_loop(0, N, body, 0)

    def meet(which):
        @pl.when(side == which)
        def _():
            pl.semaphore_wait(barrier, 3 + len(peers.get(which, [])))

    for which in range(4):
        meet(which)

    def hop(src, dst, send, recv, cc, ss):
        return pltpu.make_async_remote_copy(
            src_ref=src, dst_ref=dst, send_sem=send, recv_sem=recv,
            device_id={"circ": cc, "side": ss}, device_id_type=MESH,
        )

    def nodes_of(h):
        return pl.ds(*PIECES[h])

    def z_first(r, h):
        return r % 2 == h

    def first_hop(t, r, h, j):
        dev = jnp.where(z_first(r, h), z_dev[j], y_dev[j])
        return hop(src1.at[t, r, nodes_of(h)], dst1.at[t, j, r, nodes_of(h)],
                   send1.at[t, j, r, h], recv1.at[t, j, r, h], dev, first_side)

    def own_hop(t, r):
        return hop(src1.at[t, r], src1.at[t, r], send0.at[t, r], recv0.at[t, r], c, partner)

    def second_hop(t, r, h, j):
        dev = jnp.where(z_first(r, h), y_dev[j], z_dev[j])
        return hop(src2.at[t, r, nodes_of(h)], dst2.at[t, j, r, nodes_of(h)],
                   send2.at[t, j, r, h], recv2.at[t, j, r, h], dev, side)

    def last_hop(t, r, h, j):
        return hop(src3.at[t, r, nodes_of(h)], dst3.at[t, j, r, nodes_of(h)],
                   send3.at[t, j, r, h], recv3.at[t, j, r, h], x_dev[j], last_side)

    def pick(code, own, others):
        low = jnp.where(code == 0, own, others[0])
        high = jnp.where(code == 2, others[1], others[2])
        return jnp.where(code < 2, low, high)

    def step(t, carry):
        @pl.when(is_mortar)
        def _():
            offset = rot[t]
            k = offset // SUBSTEPS
            residue = offset - k * SUBSTEPS
            left = jnp.where(residue == 0, LEFT[0], jnp.where(residue == 1, LEFT[1], LEFT[2]))
            shifts = []
            for m in range(N):
                kappa = k + jnp.where(m < left, 1, 0)
                shifts.append(jnp.where(is_rotor, kappa, 128 * 64 - kappa) & 127)

            def send(r, carry):
                nodes = [face[r, n] for n in range(N)]
                for m in range(N):
                    total = splat[t, m * N] * nodes[0]
                    for n in range(1, N):
                        total = total + splat[t, m * N + n] * nodes[n]
                    src1[t, r, m] = pltpu.roll(total, shifts[m], 1)
                for h in range(2):
                    for j in range(3):
                        first_hop(t, r, h, j).start()

                @pl.when(side == 2)
                def _():
                    own_hop(t, r).start()

                return carry

            lax.fori_loop(0, N, send, 0)

            @pl.when(t > 0)
            def _():
                def rest(r, carry):
                    for cc in range(N):
                        d = delta[r, cc]
                        res = half_line(DERIV.T, [(edge[p] * d) * co[0, p, r, cc] for p in range(N)])
                        for a in range(N):
                            ap[a, r, cc] = ap[a, r, cc] + res[a]
                    for cc in range(N):
                        ap[fm, r, cc] = face[r, cc]
                    return carry

                lax.fori_loop(0, N, rest, 0)

        @pl.when(t == 0)
        def _():
            def first_slice(i, carry):
                a = ordered(i)
                for copy in load_slice(a):
                    copy.wait()
                in_face(a)
                return carry

            lax.fori_loop(1, N, first_slice, 0)
            lax.fori_loop(0, N, axial, 0)
            load_scale.wait()

            @pl.when(is_mortar)
            def _():
                def body(r, carry):
                    for cc in range(N):
                        total = re[fm, r, cc]
                        for p in range(N):
                            total = total + float(DERIV[p, 0]) ** 2 * jnp.where(
                                parity == 1, co[0, 6 - p, r, cc], co[0, p, r, cc]
                            )
                        diag[r, cc] = total
                    return carry

                lax.fori_loop(0, N, body, 0)

        side_copy = hop(ap.at[fp], side_dst.at[t], side_send.at[t], side_recv.at[t], c, partner)
        side_copy.start()

        def pack(a, carry):
            low, high = carry
            for r in range(N):
                here = lane == a * N + r
                low = jnp.where(here, jnp.broadcast_to(ap[a, r, 0][:, 0:1], (8, 128)), low)
                high = jnp.where(here, jnp.broadcast_to(ap[a, r, 6][:, 127:128], (8, 128)), high)
            return low, high

        zero = jnp.zeros((8, 128), jnp.float32)
        low, high = lax.fori_loop(0, N, pack, (zero, zero))
        halo_src[t, 0] = low
        halo_src[t, 1] = high
        low_copy = hop(halo_src.at[t, 0], halo_dst.at[t, 0], halo_send.at[t, 0], halo_recv.at[t, 0], prv, side)
        high_copy = hop(halo_src.at[t, 1], halo_dst.at[t, 1], halo_send.at[t, 1], halo_recv.at[t, 1], nxt, side)
        low_copy.start()
        high_copy.start()

        @pl.when(is_relay)
        def _():
            def first_relay(r, carry):
                @pl.when(side == 3)
                def _():
                    own_hop(t, r).wait_recv()

                for h in range(2):
                    for j in range(3):
                        first_hop(t, r, h, j).wait_recv()
                    which = jnp.where(z_first(r, h), 0, 1)
                    for m in range(PIECES[h][0], sum(PIECES[h])):
                        src2[t, r, m] = pick(
                            codes[t, which, m], src1[t, r, m], [dst1[t, j, r, m] for j in range(3)]
                        )
                    for j in range(3):
                        second_hop(t, r, h, j).start()
                return carry

            lax.fori_loop(0, N, first_relay, 0)

        low_copy.wait()
        high_copy.wait()

        def advance(a, carry):
            after, before = carry
            for r in range(N):
                for cc in range(N):
                    total = ap[a, r, cc]
                    if r == 6:
                        total = total + jnp.where(row == 7, 0.0, pltpu.roll(ap[a, 0, cc], 7, 0))
                    if r == 0:
                        total = total + jnp.where(row == 0, 0.0, pltpu.roll(ap[a, 6, cc], 1, 0))
                    if cc == 6:
                        other = jnp.broadcast_to(after[:, r:r + 1], (8, 128))
                        total = total + jnp.where(lane == 127, other, pltpu.roll(ap[a, r, 0], 127, 1))
                    if cc == 0:
                        other = jnp.broadcast_to(before[:, r:r + 1], (8, 128))
                        total = total + jnp.where(lane == 0, other, pltpu.roll(ap[a, r, 6], 1, 1))
                    u[a, r, cc] = u[a, r, cc] - sc[a, r, cc] * total
            return pltpu.roll(after, 128 - N, 1), pltpu.roll(before, 128 - N, 1)

        lax.fori_loop(0, N, advance, (halo_dst[t, 0], halo_dst[t, 1]))
        side_copy.wait()

        def add_side(r, carry):
            for cc in range(N):
                u[fp, r, cc] = u[fp, r, cc] - sc[fp, r, cc] * side_dst[t, r, cc]
            return carry

        lax.fori_loop(0, N, add_side, 0)

        def relay(r, carry):
            @pl.when(is_relay)
            def _():
                for h in range(2):
                    for j in range(3):
                        second_hop(t, r, h, j).wait_recv()
                    which = jnp.where(z_first(r, h), 2, 0)
                    for m in range(PIECES[h][0], sum(PIECES[h])):
                        src3[t, r, m] = pick(
                            codes[t, which, m], src2[t, r, m], [dst2[t, j, r, m] for j in range(3)]
                        )
                    for j in range(2):
                        last_hop(t, r, h, j).start()

            @pl.when(t < STEPS - 1)
            def _():
                in_face(r)

            return carry

        lax.fori_loop(0, N, relay, 0)

        @pl.when(t < STEPS - 1)
        def _():
            lax.fori_loop(0, N, axial, 0)

        @pl.when(is_mortar)
        def _():
            def arrive(r, carry):
                for h in range(2):
                    for j in range(2):
                        last_hop(t, r, h, j).wait_recv()
                nodes = [
                    jnp.where(codes[t, 3, m] == 0, dst3[t, 0, r, m], dst3[t, 1, r, m])
                    for m in range(N)
                ]
                changes = []
                for n in range(N):
                    total = splat[t, N * N + n * N] * nodes[0]
                    for m in range(1, N):
                        total = total + splat[t, N * N + n * N + m] * nodes[m]
                    change = -(sc[fm, r, n] * total)
                    changes.append(change)
                    delta[r, n] = change
                    u[fm, r, n] = u[fm, r, n] + change

                @pl.when(t < STEPS - 1)
                def _():
                    res = apply_line(changes, [co[2, fm, r, p] for p in range(N)])
                    for n in range(N):
                        face[r, n] = ap[fm, r, n] + res[n] + diag[r, n] * changes[n]

                return carry

            lax.fori_loop(0, N, arrive, 0)

            @pl.when(t < STEPS - 1)
            def _():
                for cc in range(N):
                    line = [delta[r, cc] for r in range(N)]
                    res = apply_line(line, [co[1, fm, p, cc] for p in range(N)])
                    for r in range(N):
                        face[r, cc] = face[r, cc] + res[r]

        return carry

    lax.fori_loop(0, STEPS, step, 0)

    def drain(i, carry):
        t = i // N
        r = i % N

        @pl.when(is_mortar)
        def _():
            for h in range(2):
                for j in range(3):
                    first_hop(t, r, h, j).wait_send()

        @pl.when(side == 2)
        def _():
            own_hop(t, r).wait_send()

        @pl.when(is_relay)
        def _():
            for h in range(2):
                for j in range(3):
                    second_hop(t, r, h, j).wait_send()
                for j in range(2):
                    last_hop(t, r, h, j).wait_send()

        return carry

    lax.fori_loop(0, STEPS * N, drain, 0)


def local(field, coeffs, reaction, step_scale, rotation):
    block = field.shape[1:]
    tile = block[-2:]
    f32 = jnp.float32
    dma = pltpu.SemaphoreType.DMA
    table = jnp.asarray(mortar_constants().reshape(-1))
    hbm_spec = pl.BlockSpec(memory_space=pltpu.HBM)
    smem_spec = pl.BlockSpec(memory_space=pltpu.SMEM)

    def face_buffers(*lead):
        return pltpu.VMEM((*lead, N, N, *tile), f32)

    result = pl.pallas_call(
        kernel,
        out_shape=pltpu.VMEM(block, f32),
        in_specs=[smem_spec, smem_spec, hbm_spec, hbm_spec, hbm_spec, hbm_spec],
        out_specs=pl.BlockSpec(memory_space=pltpu.VMEM),
        scratch_shapes=[
            pltpu.VMEM((3, *block), f32),
            pltpu.VMEM(block, f32),
            pltpu.VMEM(block, f32),
            pltpu.VMEM(block, f32),
            pltpu.VMEM((STEPS, 2 * N * N, *tile), f32),
            pltpu.VMEM((STEPS, 4, N, *tile), jnp.int32),
            face_buffers(),
            face_buffers(),
            face_buffers(),
            pltpu.VMEM((STEPS, 2, *tile), f32),
            pltpu.VMEM((STEPS, 2, *tile), f32),
            face_buffers(STEPS),
            face_buffers(STEPS),
            face_buffers(STEPS, 3),
            face_buffers(STEPS),
            face_buffers(STEPS, 3),
            face_buffers(STEPS),
            face_buffers(STEPS, 2),
            dma((N, 3)),
            dma((2,)),
            dma,
            dma((STEPS, 2)),
            dma((STEPS, 2)),
            dma((STEPS,)),
            dma((STEPS,)),
            dma((STEPS, N)),
            dma((STEPS, N)),
            dma((STEPS, 3, N, 2)),
            dma((STEPS, 3, N, 2)),
            dma((STEPS, 3, N, 2)),
            dma((STEPS, 3, N, 2)),
            dma((STEPS, 2, N, 2)),
            dma((STEPS, 2, N, 2)),
        ],
        compiler_params=pltpu.CompilerParams(
            collective_id=0, has_side_effects=True, vmem_limit_bytes=61 * 1024 * 1024
        ),
    )(rotation, table, field[0], coeffs[0], reaction[0], step_scale[0])
    return result[None]


def solution(mesh):
    in_specs = (
        P("side", None, None, None, None, "circ"),
        P("side", None, None, None, None, None, "circ"),
        P("side", None, None, None, None, "circ"),
        P("side", None, None, None, None, "circ"),
        P(),
    )
    out_specs = P("side", None, None, None, None, "circ")
    return jax.shard_map(local, mesh=mesh, in_specs=in_specs, out_specs=out_specs, check_vma=False)
```

```python
import jax
import jax.numpy as jnp
import numpy as np
from jax import lax
from jax.experimental import pallas as pl
from jax.experimental.pallas import tpu as pltpu
from jax.sharding import PartitionSpec as P

SUBSTEPS = 3
STEPS = 4
N = 7
NY = 4
NZ = 4
PIECES = ((0, 4), (4, 3))
MESH = pl.DeviceIdType.MESH


def gll_points():
    return np.array(
        [-1.0, -0.830223896278567, -0.4688487934707142, 0.0,
         0.4688487934707142, 0.830223896278567, 1.0]
    )


def derivative_table():
    points = gll_points()
    weights = np.array(
        [1.0 / np.prod([points[j] - points[k] for k in range(N) if k != j]) for j in range(N)]
    )
    derivative = np.zeros((N, N))
    for i in range(N):
        for j in range(N):
            if i != j:
                derivative[i, j] = weights[j] / weights[i] / (points[i] - points[j])
        derivative[i, i] = -np.sum(derivative[i])
    return derivative


def lagrange_row(location):
    points = gll_points()
    return np.array(
        [np.prod([(location - points[q]) / (points[n] - points[q]) for q in range(N) if q != n])
         for n in range(N)]
    )


def mortar_constants():
    heights = (1.0 + gll_points()) * 0.5
    table = np.zeros((2, SUBSTEPS, 2, N, N))
    for residue in range(SUBSTEPS):
        fraction = residue / SUBSTEPS
        rows = []
        for m in range(N):
            local = heights[m] - fraction
            if heights[m] < fraction:
                local += 1.0
            rows.append(lagrange_row(2.0 * local - 1.0))
        both = np.array(rows)
        table[0, residue, 0] = both
        table[0, residue, 1] = both.T
        table[1, residue, 0] = np.eye(N)
        table[1, residue, 1] = np.eye(N)
    return table.astype(np.float32)


def left_counts():
    heights = (1.0 + gll_points()) * 0.5
    return [int(np.sum(heights < residue / SUBSTEPS)) for residue in range(SUBSTEPS)]


DERIV = derivative_table()
LEFT = left_counts()


def half_line(matrix, v):
    even = [v[q] + v[6 - q] for q in range(3)]
    odd = [v[q] - v[6 - q] for q in range(3)]
    out = [None] * N
    for p in range(3):
        e = float(matrix[p, 3]) * v[3]
        o = None
        for q in range(3):
            e = e + float(0.5 * (matrix[p, q] + matrix[p, 6 - q])) * even[q]
            term = float(0.5 * (matrix[p, q] - matrix[p, 6 - q])) * odd[q]
            o = term if o is None else o + term
        out[p] = o + e
        out[6 - p] = o - e
    out[3] = (
        float(matrix[3, 0]) * odd[0] + float(matrix[3, 1]) * odd[1] + float(matrix[3, 2]) * odd[2]
    )
    return out


def apply_line(v, coeff):
    grad = half_line(DERIV, v)
    return half_line(DERIV.T, [coeff[p] * grad[p] for p in range(N)])


def kernel(
    rot, table, field, coeffs, reaction, scale, u,
    co, re, sc, ap, splat, codes, face, delta, diag,
    halo_src, halo_dst, side_dst,
    dst1, src2, dst2, src3, dst3,
    load_sem, halo_send, halo_recv, side_send, side_recv,
    sends, recv1, recv2, recv3,
):
    c = lax.axis_index("circ")
    side = lax.axis_index("side")
    count = lax.axis_size("circ")
    z_me = c % NZ
    y_me = (c // NZ) % NY
    x_me = c // (NZ * NY)
    parity = side % 2
    is_mortar = (side == 1) | (side == 2)
    is_relay = parity == 1
    is_rotor = side < 2
    partner = side + 1 - 2 * parity
    fp = 6 - 6 * parity
    fm = 6 * parity
    lane = lax.broadcasted_iota(jnp.int32, (8, 128), 1)
    row = lax.broadcasted_iota(jnp.int32, (8, 128), 0)

    def at(xx, yy, zz):
        return (xx * NY + yy) * NZ + zz

    nxt = (c + 1) % count
    prv = (c + count - 1) % count
    z_dev = [at(x_me, y_me, (z_me + j + 1) % NZ) for j in range(3)]
    y_dev = [at(x_me, (y_me + j + 1) % NY, z_me) for j in range(3)]
    x_dev = [at((x_me + j) % 2, y_me, z_me) for j in range(2)]
    first_side = jnp.where(side == 1, 1, 3)
    last_side = jnp.where(side == 1, 2, 1)

    def ordered(i):
        return jnp.where(parity == 1, 6 - i, i)

    rest_of = pl.ds(1 - parity, N - 1)
    in_layer = pl.ds(1, 2)

    def load(i, src, dst):
        return pltpu.make_async_copy(src, dst, load_sem.at[i])

    load_first = [
        load(0, field, u),
        load(1, coeffs.at[in_layer, fm], co.at[in_layer, fm]),
        load(2, reaction.at[fm], re.at[fm]),
    ]
    load_axial = load(3, coeffs.at[0], co.at[0])
    load_rest = [
        load(4, coeffs.at[in_layer, rest_of], co.at[in_layer, rest_of]),
        load(5, reaction.at[rest_of], re.at[rest_of]),
        load(6, scale, sc),
    ]

    barrier = pltpu.get_barrier_semaphore()

    def greet(cc, ss):
        pl.semaphore_signal(
            barrier, inc=1, device_id={"circ": cc, "side": ss}, device_id_type=MESH
        )

    greet(nxt, side)
    greet(prv, side)
    greet(c, partner)

    ring = z_dev + y_dev
    peers = {
        1: [(d, 1) for d in ring] + [(d, 2) for d in x_dev] + [(d, 3) for d in x_dev],
        2: [(d, 3) for d in ring] + [(d, 1) for d in x_dev],
        3: [(d, 2) for d in ring] + [(d, 3) for d in ring] + [(d, 1) for d in x_dev],
    }

    def greet_peers(which):
        @pl.when(side == which)
        def _():
            for d, ss in peers[which]:
                greet(d, ss)

    for which in peers:
        greet_peers(which)

    for copy in load_first + [load_axial] + load_rest:
        copy.start()

    def digits(shift):
        s = shift & 127
        total = ((shift >> 7) + jnp.where(lane < s, 1, 0)) & 31
        dz = total & 3
        dy = (total >> 2) & 3
        late = dy + jnp.where(z_me < dz, 1, 0)
        early = dy + jnp.where(z_me + dz > 3, 1, 0)
        dx = ((total >> 4) + jnp.where(y_me < late, 1, 0)) & 1
        return dz, early & 3, late & 3, dx

    @pl.when(side > 0)
    def _():
        def prepare(t, carry):
            offset = rot[t]
            k = offset // SUBSTEPS
            residue = offset - k * SUBSTEPS
            left = jnp.where(residue == 0, LEFT[0], jnp.where(residue == 1, LEFT[1], LEFT[2]))
            cycle = count * 128
            for m in range(N):
                kappa = k + jnp.where(m < left, 1, 0)
                kappa = jnp.where(kappa >= cycle, kappa - cycle, kappa)
                back = jnp.where(kappa == 0, 0, cycle - kappa)
                dz, early, late, _ = digits(jnp.where(is_rotor, kappa, back))
                codes[t, 0, m] = dz
                codes[t, 1, m] = early
                codes[t, 2, m] = late
                codes[t, 3, m] = digits(jnp.where(is_rotor, back, kappa))[3]
            half = jnp.where(is_rotor, 0, 1)
            first = (half * SUBSTEPS + residue) * 2 * N * N
            for i in range(2 * N * N):
                splat[t, i] = jnp.full((8, 128), table[first + i], jnp.float32)
            return carry

        lax.fori_loop(0, STEPS, prepare, 0)

    def in_face(a):
        for cc in range(N):
            line = [u[a, r, cc] for r in range(N)]
            res = apply_line(line, [co[1, a, p, cc] for p in range(N)])
            for r in range(N):
                ap[a, r, cc] = res[r] + re[a, r, cc] * line[r]
        for r in range(N):
            line = [u[a, r, cc] for cc in range(N)]
            res = apply_line(line, [co[2, a, r, p] for p in range(N)])
            for cc in range(N):
                ap[a, r, cc] = ap[a, r, cc] + res[cc]

    def axial(r, carry):
        for cc in range(N):
            line = [u[a, r, cc] for a in range(N)]
            res = apply_line(line, [co[0, p, r, cc] for p in range(N)])
            for a in range(N):
                ap[a, r, cc] = ap[a, r, cc] + res[a]
        return carry

    def next_slice(a, carry):
        in_face(a)
        return carry

    edge = [jnp.where(parity == 1, float(DERIV[p, 6]), float(DERIV[p, 0])) for p in range(N)]

    for copy in load_first:
        copy.wait()
    in_face(fm)
    load_axial.wait()

    @pl.when(is_mortar)
    def _():
        def body(r, carry):
            for cc in range(N):
                grad = half_line(DERIV, [u[a, r, cc] for a in range(N)])
                total = ap[fm, r, cc]
                for p in range(N):
                    total = total + edge[p] * (co[0, p, r, cc] * grad[p])
                face[r, cc] = total
            return carry

        lax.fori_loop(0, N, body, 0)

    def meet(which):
        @pl.when(side == which)
        def _():
            pl.semaphore_wait(barrier, 3 + len(peers.get(which, [])))

    for which in range(4):
        meet(which)

    def hop(src, dst, send, recv, cc, ss):
        return pltpu.make_async_remote_copy(
            src_ref=src, dst_ref=dst, send_sem=send, recv_sem=recv,
            device_id={"circ": cc, "side": ss}, device_id_type=MESH,
        )

    def nodes_of(h):
        return pl.ds(*PIECES[h])

    def z_first(r, h):
        return r % 2 == h

    def first_hop(t, r, h, j):
        dev = jnp.where(z_first(r, h), z_dev[j], y_dev[j])
        return hop(dst1.at[t, 3, r, nodes_of(h)], dst1.at[t, j, r, nodes_of(h)],
                   sends.at[0], recv1.at[t % 2, r, h], dev, first_side)

    def own_hop(t, r, h):
        return hop(dst1.at[t, 3, r, nodes_of(h)], dst1.at[t, 3, r, nodes_of(h)],
                   sends.at[1], recv1.at[t % 2, r, h], c, partner)

    def second_hop(t, r, h, j):
        dev = jnp.where(z_first(r, h), y_dev[j], z_dev[j])
        return hop(src2.at[t, r, nodes_of(h)], dst2.at[t, j, r, nodes_of(h)],
                   sends.at[2], recv2.at[t % 2, r, h], dev, side)

    def last_hop(t, r, h, j):
        return hop(src3.at[t, r, nodes_of(h)], dst3.at[t, j, r, nodes_of(h)],
                   sends.at[3], recv3.at[t % 2, r], x_dev[j], last_side)

    def landed(ref, sem):
        hop(ref, ref, sends.at[0], sem, c, partner).wait_recv()

    def sent(ref, i):
        hop(ref, ref, sends.at[i], recv3.at[0, 0], c, partner).wait_send()

    def pick(code, own, others):
        low = jnp.where(code == 0, own, others[0])
        high = jnp.where(code == 2, others[1], others[2])
        return jnp.where(code < 2, low, high)

    def step(t, carry):
        @pl.when(is_mortar)
        def _():
            offset = rot[t]
            k = offset // SUBSTEPS
            residue = offset - k * SUBSTEPS
            left = jnp.where(residue == 0, LEFT[0], jnp.where(residue == 1, LEFT[1], LEFT[2]))
            shifts = []
            for m in range(N):
                kappa = k + jnp.where(m < left, 1, 0)
                shifts.append(jnp.where(is_rotor, kappa, 128 * 64 - kappa) & 127)

            def send(r, carry):
                nodes = [face[r, n] for n in range(N)]
                for m in range(N):
                    total = splat[t, m * N] * nodes[0]
                    for n in range(1, N):
                        total = total + splat[t, m * N + n] * nodes[n]
                    dst1[t, 3, r, m] = pltpu.roll(total, shifts[m], 1)
                for h in range(2):
                    for j in range(3):
                        first_hop(t, r, h, j).start()

                @pl.when(side == 2)
                def _():
                    for h in range(2):
                        own_hop(t, r, h).start()

                return carry

            lax.fori_loop(0, N, send, 0)

            @pl.when(t > 0)
            def _():
                def rest(r, carry):
                    for cc in range(N):
                        d = delta[r, cc]
                        res = half_line(DERIV.T, [(edge[p] * d) * co[0, p, r, cc] for p in range(N)])
                        for a in range(N):
                            ap[a, r, cc] = ap[a, r, cc] + res[a]
                    for cc in range(N):
                        ap[fm, r, cc] = face[r, cc]
                    return carry

                lax.fori_loop(0, N, rest, 0)

        @pl.when(t == 0)
        def _():
            for copy in load_rest:
                copy.wait()

            def first_slice(i, carry):
                in_face(ordered(i))
                return carry

            lax.fori_loop(1, N, first_slice, 0)
            lax.fori_loop(0, N, axial, 0)

            @pl.when(is_mortar)
            def _():
                def body(r, carry):
                    for cc in range(N):
                        total = re[fm, r, cc]
                        for p in range(N):
                            total = total + float(DERIV[p, 0]) ** 2 * jnp.where(
                                parity == 1, co[0, 6 - p, r, cc], co[0, p, r, cc]
                            )
                        diag[r, cc] = total
                    return carry

                lax.fori_loop(0, N, body, 0)

        side_copy = hop(ap.at[fp], side_dst.at[t], side_send, side_recv.at[t % 2], c, partner)
        side_copy.start()

        def pack(a, carry):
            low, high = carry
            for r in range(N):
                here = lane == a * N + r
                low = jnp.where(here, jnp.broadcast_to(ap[a, r, 0][:, 0:1], (8, 128)), low)
                high = jnp.where(here, jnp.broadcast_to(ap[a, r, 6][:, 127:128], (8, 128)), high)
            return low, high

        zero = jnp.zeros((8, 128), jnp.float32)
        low, high = lax.fori_loop(0, N, pack, (zero, zero))
        halo_src[t, 0] = low
        halo_src[t, 1] = high
        low_copy = hop(halo_src.at[t, 0], halo_dst.at[t, 0], halo_send.at[0], halo_recv.at[t % 2, 0], prv, side)
        high_copy = hop(halo_src.at[t, 1], halo_dst.at[t, 1], halo_send.at[1], halo_recv.at[t % 2, 1], nxt, side)
        low_copy.start()
        high_copy.start()

        @pl.when(is_relay)
        def _():
            def first_relay(r, carry):
                for h in range(2):
                    @pl.when(side == 3)
                    def _():
                        landed(dst1.at[t, pl.ds(0, 4), r, nodes_of(h)], recv1.at[t % 2, r, h])

                    @pl.when(side == 1)
                    def _():
                        landed(dst1.at[t, pl.ds(0, 3), r, nodes_of(h)], recv1.at[t % 2, r, h])

                    which = jnp.where(z_first(r, h), 0, 1)
                    for m in range(PIECES[h][0], sum(PIECES[h])):
                        src2[t, r, m] = pick(
                            codes[t, which, m], dst1[t, 3, r, m], [dst1[t, j, r, m] for j in range(3)]
                        )
                    for j in range(3):
                        second_hop(t, r, h, j).start()
                return carry

            lax.fori_loop(0, N, first_relay, 0)

        low_copy.wait()
        high_copy.wait()

        def advance(a, carry):
            after, before = carry
            for r in range(N):
                for cc in range(N):
                    total = ap[a, r, cc]
                    if r == 6:
                        total = total + jnp.where(row == 7, 0.0, pltpu.roll(ap[a, 0, cc], 7, 0))
                    if r == 0:
                        total = total + jnp.where(row == 0, 0.0, pltpu.roll(ap[a, 6, cc], 1, 0))
                    if cc == 6:
                        other = jnp.broadcast_to(after[:, r:r + 1], (8, 128))
                        total = total + jnp.where(lane == 127, other, pltpu.roll(ap[a, r, 0], 127, 1))
                    if cc == 0:
                        other = jnp.broadcast_to(before[:, r:r + 1], (8, 128))
                        total = total + jnp.where(lane == 0, other, pltpu.roll(ap[a, r, 6], 1, 1))
                    u[a, r, cc] = u[a, r, cc] - sc[a, r, cc] * total
            return pltpu.roll(after, 128 - N, 1), pltpu.roll(before, 128 - N, 1)

        lax.fori_loop(0, N, advance, (halo_dst[t, 0], halo_dst[t, 1]))
        side_copy.wait()

        def add_side(r, carry):
            for cc in range(N):
                u[fp, r, cc] = u[fp, r, cc] - sc[fp, r, cc] * side_dst[t, r, cc]
            return carry

        lax.fori_loop(0, N, add_side, 0)

        def relay(r, carry):
            @pl.when(is_relay)
            def _():
                for h in range(2):
                    landed(dst2.at[t, pl.ds(0, 3), r, nodes_of(h)], recv2.at[t % 2, r, h])
                    which = jnp.where(z_first(r, h), 2, 0)
                    for m in range(PIECES[h][0], sum(PIECES[h])):
                        src3[t, r, m] = pick(
                            codes[t, which, m], src2[t, r, m], [dst2[t, j, r, m] for j in range(3)]
                        )
                    for j in range(2):
                        last_hop(t, r, h, j).start()

            @pl.when(t < STEPS - 1)
            def _():
                in_face(r)

            return carry

        lax.fori_loop(0, N, relay, 0)

        @pl.when(t < STEPS - 1)
        def _():
            lax.fori_loop(0, N, axial, 0)

        @pl.when(is_mortar)
        def _():
            def arrive(r, carry):
                landed(dst3.at[t, pl.ds(0, 2), r], recv3.at[t % 2, r])
                nodes = [
                    jnp.where(codes[t, 3, m] == 0, dst3[t, 0, r, m], dst3[t, 1, r, m])
                    for m in range(N)
                ]
                changes = []
                for n in range(N):
                    total = splat[t, N * N + n * N] * nodes[0]
                    for m in range(1, N):
                        total = total + splat[t, N * N + n * N + m] * nodes[m]
                    change = -(sc[fm, r, n] * total)
                    changes.append(change)
                    delta[r, n] = change
                    u[fm, r, n] = u[fm, r, n] + change

                @pl.when(t < STEPS - 1)
                def _():
                    res = apply_line(changes, [co[2, fm, r, p] for p in range(N)])
                    for n in range(N):
                        face[r, n] = ap[fm, r, n] + res[n] + diag[r, n] * changes[n]

                return carry

            lax.fori_loop(0, N, arrive, 0)

            @pl.when(t < STEPS - 1)
            def _():
                for cc in range(N):
                    line = [delta[r, cc] for r in range(N)]
                    res = apply_line(line, [co[1, fm, p, cc] for p in range(N)])
                    for r in range(N):
                        face[r, cc] = face[r, cc] + res[r]

        return carry

    lax.fori_loop(0, STEPS, step, 0)

    every = pl.ds(0, STEPS)

    @pl.when(is_mortar)
    def _():
        sent(dst1.at[every, pl.ds(0, 3)], 0)

    @pl.when(side == 2)
    def _():
        sent(dst1.at[every, 3], 1)

    @pl.when(is_relay)
    def _():
        sent(dst2, 2)
        sent(dst3, 3)


def local(field, coeffs, reaction, step_scale, rotation):
    block = field.shape[1:]
    tile = block[-2:]
    f32 = jnp.float32
    dma = pltpu.SemaphoreType.DMA
    table = jnp.asarray(mortar_constants().reshape(-1))
    hbm_spec = pl.BlockSpec(memory_space=pltpu.HBM)
    smem_spec = pl.BlockSpec(memory_space=pltpu.SMEM)

    def face_buffers(*lead):
        return pltpu.VMEM((*lead, N, N, *tile), f32)

    result = pl.pallas_call(
        kernel,
        out_shape=pltpu.VMEM(block, f32),
        in_specs=[smem_spec, smem_spec, hbm_spec, hbm_spec, hbm_spec, hbm_spec],
        out_specs=pl.BlockSpec(memory_space=pltpu.VMEM),
        scratch_shapes=[
            pltpu.VMEM((3, *block), f32),
            pltpu.VMEM(block, f32),
            pltpu.VMEM(block, f32),
            pltpu.VMEM(block, f32),
            pltpu.VMEM((STEPS, 2 * N * N, *tile), f32),
            pltpu.VMEM((STEPS, 4, N, *tile), jnp.int32),
            face_buffers(),
            face_buffers(),
            face_buffers(),
            pltpu.VMEM((STEPS, 2, *tile), f32),
            pltpu.VMEM((STEPS, 2, *tile), f32),
            face_buffers(STEPS),
            face_buffers(STEPS, 4),
            face_buffers(STEPS),
            face_buffers(STEPS, 3),
            face_buffers(STEPS),
            face_buffers(STEPS, 2),
            dma((7,)),
            dma((2,)),
            dma((2, 2)),
            dma,
            dma((2,)),
            dma((4,)),
            dma((2, N, 2)),
            dma((2, N, 2)),
            dma((2, N)),
        ],
        compiler_params=pltpu.CompilerParams(
            collective_id=0, has_side_effects=True, vmem_limit_bytes=61 * 1024 * 1024
        ),
    )(rotation, table, field[0], coeffs[0], reaction[0], step_scale[0])
    return result[None]


def solution(mesh):
    in_specs = (
        P("side", None, None, None, None, "circ"),
        P("side", None, None, None, None, None, "circ"),
        P("side", None, None, None, None, "circ"),
        P("side", None, None, None, None, "circ"),
        P(),
    )
    out_specs = P("side", None, None, None, None, "circ")
    return jax.shard_map(local, mesh=mesh, in_specs=in_specs, out_specs=out_specs, check_vma=False)
```

```python
import jax
import jax.numpy as jnp
import numpy as np
from jax import lax
from jax.experimental import pallas as pl
from jax.experimental.pallas import tpu as pltpu
from jax.sharding import PartitionSpec as P

SUBSTEPS = 3
STEPS = 4
N = 7
NY = 4
NZ = 4
PIECES = ((0, 4), (4, 3))
MESH = pl.DeviceIdType.MESH


def gll_points():
    return np.array(
        [-1.0, -0.830223896278567, -0.4688487934707142, 0.0,
         0.4688487934707142, 0.830223896278567, 1.0]
    )


def derivative_table():
    points = gll_points()
    weights = np.array(
        [1.0 / np.prod([points[j] - points[k] for k in range(N) if k != j]) for j in range(N)]
    )
    derivative = np.zeros((N, N))
    for i in range(N):
        for j in range(N):
            if i != j:
                derivative[i, j] = weights[j] / weights[i] / (points[i] - points[j])
        derivative[i, i] = -np.sum(derivative[i])
    return derivative


def lagrange_row(location):
    points = gll_points()
    return np.array(
        [np.prod([(location - points[q]) / (points[n] - points[q]) for q in range(N) if q != n])
         for n in range(N)]
    )


def mortar_constants():
    heights = (1.0 + gll_points()) * 0.5
    table = np.zeros((2, SUBSTEPS, 2, N, N))
    for residue in range(SUBSTEPS):
        fraction = residue / SUBSTEPS
        rows = []
        for m in range(N):
            local = heights[m] - fraction
            if heights[m] < fraction:
                local += 1.0
            rows.append(lagrange_row(2.0 * local - 1.0))
        both = np.array(rows)
        table[0, residue, 0] = both
        table[0, residue, 1] = both.T
        table[1, residue, 0] = np.eye(N)
        table[1, residue, 1] = np.eye(N)
    return table.astype(np.float32)


def left_counts():
    heights = (1.0 + gll_points()) * 0.5
    return [int(np.sum(heights < residue / SUBSTEPS)) for residue in range(SUBSTEPS)]


DERIV = derivative_table()
LEFT = left_counts()


def half_line(matrix, v):
    even = [v[q] + v[6 - q] for q in range(3)]
    odd = [v[q] - v[6 - q] for q in range(3)]
    out = [None] * N
    for p in range(3):
        e = float(matrix[p, 3]) * v[3]
        o = None
        for q in range(3):
            e = e + float(0.5 * (matrix[p, q] + matrix[p, 6 - q])) * even[q]
            term = float(0.5 * (matrix[p, q] - matrix[p, 6 - q])) * odd[q]
            o = term if o is None else o + term
        out[p] = o + e
        out[6 - p] = o - e
    out[3] = (
        float(matrix[3, 0]) * odd[0] + float(matrix[3, 1]) * odd[1] + float(matrix[3, 2]) * odd[2]
    )
    return out


def apply_line(v, coeff):
    grad = half_line(DERIV, v)
    return half_line(DERIV.T, [coeff[p] * grad[p] for p in range(N)])


def kernel(
    rot, table, field, coeffs, reaction, scale, u,
    co, re, sc, ap, splat, codes, face, delta, diag,
    halo_src, halo_dst, side_dst,
    dst1, src2, dst2, src3, dst3,
    load_sem, halo_send, halo_recv, side_send, side_recv,
    sends, recv1, recv2, recv3,
):
    c = lax.axis_index("circ")
    side = lax.axis_index("side")
    count = lax.axis_size("circ")
    z_me = c % NZ
    y_me = (c // NZ) % NY
    x_me = c // (NZ * NY)
    parity = side % 2
    is_mortar = (side == 1) | (side == 2)
    is_relay = parity == 1
    is_rotor = side < 2
    partner = side + 1 - 2 * parity
    fp = 6 - 6 * parity
    fm = 6 * parity
    lane = lax.broadcasted_iota(jnp.int32, (8, 128), 1)
    row = lax.broadcasted_iota(jnp.int32, (8, 128), 0)

    def at(xx, yy, zz):
        return (xx * NY + yy) * NZ + zz

    nxt = (c + 1) % count
    prv = (c + count - 1) % count
    z_dev = [at(x_me, y_me, (z_me + j + 1) % NZ) for j in range(3)]
    y_dev = [at(x_me, (y_me + j + 1) % NY, z_me) for j in range(3)]
    x_dev = [at((x_me + j) % 2, y_me, z_me) for j in range(2)]
    first_side = jnp.where(side == 1, 1, 3)
    last_side = jnp.where(side == 1, 2, 1)

    def ordered(i):
        return jnp.where(parity == 1, 6 - i, i)

    rest_of = pl.ds(1 - parity, N - 1)
    in_layer = pl.ds(1, 2)

    def load(i, src, dst):
        return pltpu.make_async_copy(src, dst, load_sem.at[i])

    load_first = [
        load(0, field, u),
        load(1, coeffs.at[in_layer, fm], co.at[in_layer, fm]),
        load(2, reaction.at[fm], re.at[fm]),
    ]
    load_axial = load(3, coeffs.at[0], co.at[0])
    load_rest = [
        load(4, coeffs.at[in_layer, rest_of], co.at[in_layer, rest_of]),
        load(5, reaction.at[rest_of], re.at[rest_of]),
        load(6, scale, sc),
    ]

    barrier = pltpu.get_barrier_semaphore()

    def greet(cc, ss):
        pl.semaphore_signal(
            barrier, inc=1, device_id={"circ": cc, "side": ss}, device_id_type=MESH
        )

    greet(nxt, side)
    greet(prv, side)
    greet(c, partner)

    ring = z_dev + y_dev
    peers = {
        1: [(d, 1) for d in ring] + [(d, 2) for d in x_dev] + [(d, 3) for d in x_dev],
        2: [(d, 3) for d in ring] + [(d, 1) for d in x_dev],
        3: [(d, 2) for d in ring] + [(d, 3) for d in ring] + [(d, 1) for d in x_dev],
    }

    def greet_peers(which):
        @pl.when(side == which)
        def _():
            for d, ss in peers[which]:
                greet(d, ss)

    for which in peers:
        greet_peers(which)

    for copy in load_first + [load_axial] + load_rest:
        copy.start()

    def digits(shift):
        s = shift & 127
        total = ((shift >> 7) + jnp.where(lane < s, 1, 0)) & 31
        dz = total & 3
        dy = (total >> 2) & 3
        late = dy + jnp.where(z_me < dz, 1, 0)
        early = dy + jnp.where(z_me + dz > 3, 1, 0)
        dx = ((total >> 4) + jnp.where(y_me < late, 1, 0)) & 1
        return dz, early & 3, late & 3, dx

    @pl.when(side > 0)
    def _():
        def prepare(t, carry):
            offset = rot[t]
            k = offset // SUBSTEPS
            residue = offset - k * SUBSTEPS
            left = jnp.where(residue == 0, LEFT[0], jnp.where(residue == 1, LEFT[1], LEFT[2]))
            cycle = count * 128
            for m in range(N):
                kappa = k + jnp.where(m < left, 1, 0)
                kappa = jnp.where(kappa >= cycle, kappa - cycle, kappa)
                back = jnp.where(kappa == 0, 0, cycle - kappa)
                dz, early, late, _ = digits(jnp.where(is_rotor, kappa, back))
                codes[t, 0, m] = dz
                codes[t, 1, m] = early
                codes[t, 2, m] = late
                codes[t, 3, m] = digits(jnp.where(is_rotor, back, kappa))[3]
            half = jnp.where(is_rotor, 0, 1)
            first = (half * SUBSTEPS + residue) * 2 * N * N
            for i in range(2 * N * N):
                splat[t, i] = jnp.full((8, 128), table[first + i], jnp.float32)
            return carry

        lax.fori_loop(0, STEPS, prepare, 0)

    def in_face(a):
        for cc in range(N):
            line = [u[a, r, cc] for r in range(N)]
            res = apply_line(line, [co[1, a, p, cc] for p in range(N)])
            for r in range(N):
                ap[a, r, cc] = res[r] + re[a, r, cc] * line[r]
        for r in range(N):
            line = [u[a, r, cc] for cc in range(N)]
            res = apply_line(line, [co[2, a, r, p] for p in range(N)])
            for cc in range(N):
                ap[a, r, cc] = ap[a, r, cc] + res[cc]

    def axial(r, carry):
        for cc in range(N):
            line = [u[a, r, cc] for a in range(N)]
            res = apply_line(line, [co[0, p, r, cc] for p in range(N)])
            for a in range(N):
                ap[a, r, cc] = ap[a, r, cc] + res[a]
        return carry

    def next_slice(a, carry):
        in_face(a)
        return carry

    edge = [jnp.where(parity == 1, float(DERIV[p, 6]), float(DERIV[p, 0])) for p in range(N)]

    for copy in load_first:
        copy.wait()
    in_face(fm)
    load_axial.wait()

    def first_face():
        def body(r, carry):
            for cc in range(N):
                grad = half_line(DERIV, [u[a, r, cc] for a in range(N)])
                total = ap[fm, r, cc]
                for p in range(N):
                    total = total + edge[p] * (co[0, p, r, cc] * grad[p])
                face[r, cc] = total
            return carry

        lax.fori_loop(0, N, body, 0)

    @pl.when(is_mortar)
    def _():
        first_face()

    def meet(which):
        @pl.when(side == which)
        def _():
            pl.semaphore_wait(barrier, 3 + len(peers.get(which, [])))

    for which in range(4):
        meet(which)

    def hop(src, dst, send, recv, cc, ss):
        return pltpu.make_async_remote_copy(
            src_ref=src, dst_ref=dst, send_sem=send, recv_sem=recv,
            device_id={"circ": cc, "side": ss}, device_id_type=MESH,
        )

    def nodes_of(h):
        return pl.ds(*PIECES[h])

    def z_first(r, h):
        return r % 2 == h

    def first_hop(t, r, h, j):
        dev = jnp.where(z_first(r, h), z_dev[j], y_dev[j])
        return hop(dst1.at[t, 3, r, nodes_of(h)], dst1.at[t, j, r, nodes_of(h)],
                   sends.at[0], recv1.at[t % 2, r, h], dev, first_side)

    def own_hop(t, r, h):
        return hop(dst1.at[t, 3, r, nodes_of(h)], dst1.at[t, 3, r, nodes_of(h)],
                   sends.at[1], recv1.at[t % 2, r, h], c, partner)

    def second_hop(t, r, h, j):
        dev = jnp.where(z_first(r, h), y_dev[j], z_dev[j])
        return hop(src2.at[t, r, nodes_of(h)], dst2.at[t, j, r, nodes_of(h)],
                   sends.at[2], recv2.at[t % 2, r, h], dev, side)

    def last_hop(t, r, h, j):
        return hop(src3.at[t, r, nodes_of(h)], dst3.at[t, j, r, nodes_of(h)],
                   sends.at[3], recv3.at[t % 2, r], x_dev[j], last_side)

    def landed(ref, sem):
        hop(ref, ref, sends.at[0], sem, c, partner).wait_recv()

    def sent(ref, i):
        hop(ref, ref, sends.at[i], recv3.at[0, 0], c, partner).wait_send()

    def pick(code, own, others):
        low = jnp.where(code == 0, own, others[0])
        high = jnp.where(code == 2, others[1], others[2])
        return jnp.where(code < 2, low, high)

    def step(t, carry):
        @pl.when(is_mortar)
        def _():
            offset = rot[t]
            k = offset // SUBSTEPS
            residue = offset - k * SUBSTEPS
            left = jnp.where(residue == 0, LEFT[0], jnp.where(residue == 1, LEFT[1], LEFT[2]))
            shifts = []
            for m in range(N):
                kappa = k + jnp.where(m < left, 1, 0)
                shifts.append(jnp.where(is_rotor, kappa, 128 * 64 - kappa) & 127)

            def send(r, carry):
                nodes = [face[r, n] for n in range(N)]
                for m in range(N):
                    total = splat[t, m * N] * nodes[0]
                    for n in range(1, N):
                        total = total + splat[t, m * N + n] * nodes[n]
                    dst1[t, 3, r, m] = pltpu.roll(total, shifts[m], 1)
                for h in range(2):
                    for j in range(3):
                        first_hop(t, r, h, j).start()

                @pl.when(side == 2)
                def _():
                    for h in range(2):
                        own_hop(t, r, h).start()

                return carry

            lax.fori_loop(0, N, send, 0)

        @pl.when(t == 0)
        def _():
            for copy in load_rest:
                copy.wait()

            @pl.when(is_mortar)
            def _():
                def body(r, carry):
                    for cc in range(N):
                        total = re[fm, r, cc]
                        for p in range(N):
                            total = total + float(DERIV[p, 0]) ** 2 * jnp.where(
                                parity == 1, co[0, 6 - p, r, cc], co[0, p, r, cc]
                            )
                        diag[r, cc] = total
                    return carry

                lax.fori_loop(0, N, body, 0)

        lax.fori_loop(0, N, next_slice, 0)
        lax.fori_loop(0, N, axial, 0)

        side_copy = hop(ap.at[fp], side_dst.at[t], side_send, side_recv.at[t % 2], c, partner)
        side_copy.start()

        def pack(a, carry):
            low, high = carry
            for r in range(N):
                here = lane == a * N + r
                low = jnp.where(here, jnp.broadcast_to(ap[a, r, 0][:, 0:1], (8, 128)), low)
                high = jnp.where(here, jnp.broadcast_to(ap[a, r, 6][:, 127:128], (8, 128)), high)
            return low, high

        zero = jnp.zeros((8, 128), jnp.float32)
        low, high = lax.fori_loop(0, N, pack, (zero, zero))
        halo_src[t, 0] = low
        halo_src[t, 1] = high
        low_copy = hop(halo_src.at[t, 0], halo_dst.at[t, 0], halo_send.at[0], halo_recv.at[t % 2, 0], prv, side)
        high_copy = hop(halo_src.at[t, 1], halo_dst.at[t, 1], halo_send.at[1], halo_recv.at[t % 2, 1], nxt, side)
        low_copy.start()
        high_copy.start()

        @pl.when(is_relay)
        def _():
            def first_relay(r, carry):
                for h in range(2):
                    @pl.when(side == 3)
                    def _():
                        landed(dst1.at[t, pl.ds(0, 4), r, nodes_of(h)], recv1.at[t % 2, r, h])

                    @pl.when(side == 1)
                    def _():
                        landed(dst1.at[t, pl.ds(0, 3), r, nodes_of(h)], recv1.at[t % 2, r, h])

                    which = jnp.where(z_first(r, h), 0, 1)
                    for m in range(PIECES[h][0], sum(PIECES[h])):
                        src2[t, r, m] = pick(
                            codes[t, which, m], dst1[t, 3, r, m], [dst1[t, j, r, m] for j in range(3)]
                        )
                    for j in range(3):
                        second_hop(t, r, h, j).start()
                return carry

            lax.fori_loop(0, N, first_relay, 0)

        def relay(r, carry):
            @pl.when(is_relay)
            def _():
                for h in range(2):
                    landed(dst2.at[t, pl.ds(0, 3), r, nodes_of(h)], recv2.at[t % 2, r, h])
                    which = jnp.where(z_first(r, h), 2, 0)
                    for m in range(PIECES[h][0], sum(PIECES[h])):
                        src3[t, r, m] = pick(
                            codes[t, which, m], src2[t, r, m], [dst2[t, j, r, m] for j in range(3)]
                        )
                    for j in range(2):
                        last_hop(t, r, h, j).start()

            return carry

        lax.fori_loop(0, N, relay, 0)

        low_copy.wait()
        high_copy.wait()

        def advance(a, carry):
            after, before = carry
            for r in range(N):
                for cc in range(N):
                    total = ap[a, r, cc]
                    if r == 6:
                        total = total + jnp.where(row == 7, 0.0, pltpu.roll(ap[a, 0, cc], 7, 0))
                    if r == 0:
                        total = total + jnp.where(row == 0, 0.0, pltpu.roll(ap[a, 6, cc], 1, 0))
                    if cc == 6:
                        other = jnp.broadcast_to(after[:, r:r + 1], (8, 128))
                        total = total + jnp.where(lane == 127, other, pltpu.roll(ap[a, r, 0], 127, 1))
                    if cc == 0:
                        other = jnp.broadcast_to(before[:, r:r + 1], (8, 128))
                        total = total + jnp.where(lane == 0, other, pltpu.roll(ap[a, r, 6], 1, 1))
                    u[a, r, cc] = u[a, r, cc] - sc[a, r, cc] * total
            return pltpu.roll(after, 128 - N, 1), pltpu.roll(before, 128 - N, 1)

        lax.fori_loop(0, N, advance, (halo_dst[t, 0], halo_dst[t, 1]))
        side_copy.wait()

        def add_side(r, carry):
            for cc in range(N):
                u[fp, r, cc] = u[fp, r, cc] - sc[fp, r, cc] * side_dst[t, r, cc]
            return carry

        lax.fori_loop(0, N, add_side, 0)


        @pl.when(is_mortar & (t < STEPS - 1))
        def _():
            in_face(fm)
            first_face()

        @pl.when(is_mortar)
        def _():
            def arrive(r, carry):
                landed(dst3.at[t, pl.ds(0, 2), r], recv3.at[t % 2, r])
                nodes = [
                    jnp.where(codes[t, 3, m] == 0, dst3[t, 0, r, m], dst3[t, 1, r, m])
                    for m in range(N)
                ]
                changes = []
                for n in range(N):
                    total = splat[t, N * N + n * N] * nodes[0]
                    for m in range(1, N):
                        total = total + splat[t, N * N + n * N + m] * nodes[m]
                    change = -(sc[fm, r, n] * total)
                    changes.append(change)
                    delta[r, n] = change
                    u[fm, r, n] = u[fm, r, n] + change

                @pl.when(t < STEPS - 1)
                def _():
                    res = apply_line(changes, [co[2, fm, r, p] for p in range(N)])
                    for n in range(N):
                        face[r, n] = face[r, n] + res[n] + diag[r, n] * changes[n]

                return carry

            lax.fori_loop(0, N, arrive, 0)

            @pl.when(t < STEPS - 1)
            def _():
                for cc in range(N):
                    line = [delta[r, cc] for r in range(N)]
                    res = apply_line(line, [co[1, fm, p, cc] for p in range(N)])
                    for r in range(N):
                        face[r, cc] = face[r, cc] + res[r]

        return carry

    lax.fori_loop(0, STEPS, step, 0)

    every = pl.ds(0, STEPS)

    @pl.when(is_mortar)
    def _():
        sent(dst1.at[every, pl.ds(0, 3)], 0)

    @pl.when(side == 2)
    def _():
        sent(dst1.at[every, 3], 1)

    @pl.when(is_relay)
    def _():
        sent(dst2, 2)
        sent(dst3, 3)


def local(field, coeffs, reaction, step_scale, rotation):
    block = field.shape[1:]
    tile = block[-2:]
    f32 = jnp.float32
    dma = pltpu.SemaphoreType.DMA
    table = jnp.asarray(mortar_constants().reshape(-1))
    hbm_spec = pl.BlockSpec(memory_space=pltpu.HBM)
    smem_spec = pl.BlockSpec(memory_space=pltpu.SMEM)

    def face_buffers(*lead):
        return pltpu.VMEM((*lead, N, N, *tile), f32)

    result = pl.pallas_call(
        kernel,
        out_shape=pltpu.VMEM(block, f32),
        in_specs=[smem_spec, smem_spec, hbm_spec, hbm_spec, hbm_spec, hbm_spec],
        out_specs=pl.BlockSpec(memory_space=pltpu.VMEM),
        scratch_shapes=[
            pltpu.VMEM((3, *block), f32),
            pltpu.VMEM(block, f32),
            pltpu.VMEM(block, f32),
            pltpu.VMEM(block, f32),
            pltpu.VMEM((STEPS, 2 * N * N, *tile), f32),
            pltpu.VMEM((STEPS, 4, N, *tile), jnp.int32),
            face_buffers(),
            face_buffers(),
            face_buffers(),
            pltpu.VMEM((STEPS, 2, *tile), f32),
            pltpu.VMEM((STEPS, 2, *tile), f32),
            face_buffers(STEPS),
            face_buffers(STEPS, 4),
            face_buffers(STEPS),
            face_buffers(STEPS, 3),
            face_buffers(STEPS),
            face_buffers(STEPS, 2),
            dma((7,)),
            dma((2,)),
            dma((2, 2)),
            dma,
            dma((2,)),
            dma((4,)),
            dma((2, N, 2)),
            dma((2, N, 2)),
            dma((2, N)),
        ],
        compiler_params=pltpu.CompilerParams(
            collective_id=0, has_side_effects=True, vmem_limit_bytes=61 * 1024 * 1024
        ),
    )(rotation, table, field[0], coeffs[0], reaction[0], step_scale[0])
    return result[None]


def solution(mesh):
    in_specs = (
        P("side", None, None, None, None, "circ"),
        P("side", None, None, None, None, None, "circ"),
        P("side", None, None, None, None, "circ"),
        P("side", None, None, None, None, "circ"),
        P(),
    )
    out_specs = P("side", None, None, None, None, "circ")
    return jax.shard_map(local, mesh=mesh, in_specs=in_specs, out_specs=out_specs, check_vma=False)
```

```python
import jax
import jax.numpy as jnp
import numpy as np
from jax import lax
from jax.experimental import pallas as pl
from jax.experimental.pallas import tpu as pltpu
from jax.sharding import PartitionSpec as P

SUBSTEPS = 3
STEPS = 4
N = 7
NY = 4
NZ = 4
PIECES = ((0, 4), (4, 3))
MESH = pl.DeviceIdType.MESH


def gll_points():
    return np.array(
        [-1.0, -0.830223896278567, -0.4688487934707142, 0.0,
         0.4688487934707142, 0.830223896278567, 1.0]
    )


def derivative_table():
    points = gll_points()
    weights = np.array(
        [1.0 / np.prod([points[j] - points[k] for k in range(N) if k != j]) for j in range(N)]
    )
    derivative = np.zeros((N, N))
    for i in range(N):
        for j in range(N):
            if i != j:
                derivative[i, j] = weights[j] / weights[i] / (points[i] - points[j])
        derivative[i, i] = -np.sum(derivative[i])
    return derivative


def lagrange_row(location):
    points = gll_points()
    return np.array(
        [np.prod([(location - points[q]) / (points[n] - points[q]) for q in range(N) if q != n])
         for n in range(N)]
    )


def mortar_constants():
    heights = (1.0 + gll_points()) * 0.5
    table = np.zeros((2, SUBSTEPS, 2, N, N))
    for residue in range(SUBSTEPS):
        fraction = residue / SUBSTEPS
        rows = []
        for m in range(N):
            local = heights[m] - fraction
            if heights[m] < fraction:
                local += 1.0
            rows.append(lagrange_row(2.0 * local - 1.0))
        both = np.array(rows)
        table[0, residue, 0] = both
        table[0, residue, 1] = both.T
        table[1, residue, 0] = np.eye(N)
        table[1, residue, 1] = np.eye(N)
    return table.astype(np.float32)


def left_counts():
    heights = (1.0 + gll_points()) * 0.5
    return [int(np.sum(heights < residue / SUBSTEPS)) for residue in range(SUBSTEPS)]


DERIV = derivative_table()
LEFT = left_counts()


def half_line(matrix, v):
    even = [v[q] + v[6 - q] for q in range(3)]
    odd = [v[q] - v[6 - q] for q in range(3)]
    out = [None] * N
    for p in range(3):
        e = float(matrix[p, 3]) * v[3]
        o = None
        for q in range(3):
            e = e + float(0.5 * (matrix[p, q] + matrix[p, 6 - q])) * even[q]
            term = float(0.5 * (matrix[p, q] - matrix[p, 6 - q])) * odd[q]
            o = term if o is None else o + term
        out[p] = o + e
        out[6 - p] = o - e
    out[3] = (
        float(matrix[3, 0]) * odd[0] + float(matrix[3, 1]) * odd[1] + float(matrix[3, 2]) * odd[2]
    )
    return out


def apply_line(v, coeff):
    grad = half_line(DERIV, v)
    return half_line(DERIV.T, [coeff[p] * grad[p] for p in range(N)])


def kernel(
    rot, table, field, coeffs, reaction, scale, u,
    co, re, sc, ap, splat, codes, face, delta, diag,
    halo_src, halo_dst, side_dst,
    dst1, src2, dst2, src3, dst3,
    load_sem, halo_send, halo_recv, side_send, side_recv,
    sends, recv1, recv2, recv3,
):
    c = lax.axis_index("circ")
    side = lax.axis_index("side")
    count = lax.axis_size("circ")
    z_me = c % NZ
    y_me = (c // NZ) % NY
    x_me = c // (NZ * NY)
    parity = side % 2
    is_mortar = (side == 1) | (side == 2)
    is_relay = parity == 1
    is_rotor = side < 2
    partner = side + 1 - 2 * parity
    fp = 6 - 6 * parity
    fm = 6 * parity
    lane = lax.broadcasted_iota(jnp.int32, (8, 128), 1)
    row = lax.broadcasted_iota(jnp.int32, (8, 128), 0)

    def at(xx, yy, zz):
        return (xx * NY + yy) * NZ + zz

    nxt = (c + 1) % count
    prv = (c + count - 1) % count
    z_dev = [at(x_me, y_me, (z_me + j + 1) % NZ) for j in range(3)]
    y_dev = [at(x_me, (y_me + j + 1) % NY, z_me) for j in range(3)]
    x_dev = [at((x_me + j) % 2, y_me, z_me) for j in range(2)]
    first_side = jnp.where(side == 1, 1, 3)
    last_side = jnp.where(side == 1, 2, 1)

    def ordered(i):
        return jnp.where(parity == 1, 6 - i, i)

    rest_of = pl.ds(1 - parity, N - 1)
    in_layer = pl.ds(1, 2)

    def load(i, src, dst):
        return pltpu.make_async_copy(src, dst, load_sem.at[i])

    load_first = [
        load(0, field, u),
        load(1, coeffs.at[in_layer, fm], co.at[in_layer, fm]),
        load(2, reaction.at[fm], re.at[fm]),
    ]
    load_axial = load(3, coeffs.at[0], co.at[0])
    load_rest = [
        load(4, coeffs.at[in_layer, rest_of], co.at[in_layer, rest_of]),
        load(5, reaction.at[rest_of], re.at[rest_of]),
        load(6, scale, sc),
    ]

    barrier = pltpu.get_barrier_semaphore()

    def greet(cc, ss):
        pl.semaphore_signal(
            barrier, inc=1, device_id={"circ": cc, "side": ss}, device_id_type=MESH
        )

    greet(nxt, side)
    greet(prv, side)
    greet(c, partner)

    ring = z_dev + y_dev
    peers = {
        1: [(d, 1) for d in ring] + [(d, 2) for d in x_dev] + [(d, 3) for d in x_dev],
        2: [(d, 3) for d in ring] + [(d, 1) for d in x_dev],
        3: [(d, 2) for d in ring] + [(d, 3) for d in ring] + [(d, 1) for d in x_dev],
    }

    def greet_peers(which):
        @pl.when(side == which)
        def _():
            for d, ss in peers[which]:
                greet(d, ss)

    for which in peers:
        greet_peers(which)

    for copy in load_first + [load_axial] + load_rest:
        copy.start()

    def digits(shift):
        s = shift & 127
        total = ((shift >> 7) + jnp.where(lane < s, 1, 0)) & 31
        dz = total & 3
        dy = (total >> 2) & 3
        late = dy + jnp.where(z_me < dz, 1, 0)
        early = dy + jnp.where(z_me + dz > 3, 1, 0)
        dx = ((total >> 4) + jnp.where(y_me < late, 1, 0)) & 1
        return dz, early & 3, late & 3, dx

    @pl.when(side > 0)
    def _():
        def prepare(t, carry):
            offset = rot[t]
            k = offset // SUBSTEPS
            residue = offset - k * SUBSTEPS
            left = jnp.where(residue == 0, LEFT[0], jnp.where(residue == 1, LEFT[1], LEFT[2]))
            cycle = count * 128
            for m in range(N):
                kappa = k + jnp.where(m < left, 1, 0)
                kappa = jnp.where(kappa >= cycle, kappa - cycle, kappa)
                back = jnp.where(kappa == 0, 0, cycle - kappa)
                dz, early, late, _ = digits(jnp.where(is_rotor, kappa, back))
                codes[t, 0, m] = dz
                codes[t, 1, m] = early
                codes[t, 2, m] = late
                codes[t, 3, m] = digits(jnp.where(is_rotor, back, kappa))[3]
            half = jnp.where(is_rotor, 0, 1)
            first = (half * SUBSTEPS + residue) * 2 * N * N
            for i in range(2 * N * N):
                splat[t, i] = jnp.full((8, 128), table[first + i], jnp.float32)
            return carry

        lax.fori_loop(0, STEPS, prepare, 0)

    def in_face(a):
        for cc in range(N):
            line = [u[a, r, cc] for r in range(N)]
            res = apply_line(line, [co[1, a, p, cc] for p in range(N)])
            for r in range(N):
                ap[a, r, cc] = res[r] + re[a, r, cc] * line[r]
        for r in range(N):
            line = [u[a, r, cc] for cc in range(N)]
            res = apply_line(line, [co[2, a, r, p] for p in range(N)])
            for cc in range(N):
                ap[a, r, cc] = ap[a, r, cc] + res[cc]

    def axial(r, columns):
        for cc in columns:
            line = [u[a, r, cc] for a in range(N)]
            res = apply_line(line, [co[0, p, r, cc] for p in range(N)])
            for a in range(N):
                ap[a, r, cc] = ap[a, r, cc] + res[a]

        @pl.when(is_mortar)
        def _():
            for cc in columns:
                ap[fm, r, cc] = face[r, cc]

    def next_slice(i, carry):
        in_face(ordered(i))
        return carry

    def ends(r, carry):
        axial(r, (0, 6))
        return carry

    edge = [jnp.where(parity == 1, float(DERIV[p, 6]), float(DERIV[p, 0])) for p in range(N)]

    for copy in load_first:
        copy.wait()
    in_face(fm)
    load_axial.wait()

    def first_face():
        def body(r, carry):
            for cc in range(N):
                grad = half_line(DERIV, [u[a, r, cc] for a in range(N)])
                total = ap[fm, r, cc]
                for p in range(N):
                    total = total + edge[p] * (co[0, p, r, cc] * grad[p])
                face[r, cc] = total
            return carry

        lax.fori_loop(0, N, body, 0)

    @pl.when(is_mortar)
    def _():
        first_face()

    def meet(which):
        @pl.when(side == which)
        def _():
            pl.semaphore_wait(barrier, 3 + len(peers.get(which, [])))

    for which in range(4):
        meet(which)

    def hop(src, dst, send, recv, cc, ss):
        return pltpu.make_async_remote_copy(
            src_ref=src, dst_ref=dst, send_sem=send, recv_sem=recv,
            device_id={"circ": cc, "side": ss}, device_id_type=MESH,
        )

    def nodes_of(h):
        return pl.ds(*PIECES[h])

    def z_first(r, h):
        return r % 2 == h

    def first_hop(t, r, h, j):
        dev = jnp.where(z_first(r, h), z_dev[j], y_dev[j])
        return hop(dst1.at[t, 3, r, nodes_of(h)], dst1.at[t, j, r, nodes_of(h)],
                   sends.at[0], recv1.at[t % 2, r, h], dev, first_side)

    def own_hop(t, r, h):
        return hop(dst1.at[t, 3, r, nodes_of(h)], dst1.at[t, 3, r, nodes_of(h)],
                   sends.at[1], recv1.at[t % 2, r, h], c, partner)

    def second_hop(t, r, h, j):
        dev = jnp.where(z_first(r, h), y_dev[j], z_dev[j])
        return hop(src2.at[t, r, nodes_of(h)], dst2.at[t, j, r, nodes_of(h)],
                   sends.at[2], recv2.at[t % 2, r, h], dev, side)

    def last_hop(t, r, h, j):
        return hop(src3.at[t, r, nodes_of(h)], dst3.at[t, j, r, nodes_of(h)],
                   sends.at[3], recv3.at[t % 2, r], x_dev[j], last_side)

    def landed(ref, sem):
        hop(ref, ref, sends.at[0], sem, c, partner).wait_recv()

    def sent(ref, i):
        hop(ref, ref, sends.at[i], recv3.at[0, 0], c, partner).wait_send()

    def pick(code, own, others):
        low = jnp.where(code == 0, own, others[0])
        high = jnp.where(code == 2, others[1], others[2])
        return jnp.where(code < 2, low, high)

    def step(t, carry):
        @pl.when(is_mortar)
        def _():
            offset = rot[t]
            k = offset // SUBSTEPS
            residue = offset - k * SUBSTEPS
            left = jnp.where(residue == 0, LEFT[0], jnp.where(residue == 1, LEFT[1], LEFT[2]))
            shifts = []
            for m in range(N):
                kappa = k + jnp.where(m < left, 1, 0)
                shifts.append(jnp.where(is_rotor, kappa, 128 * 64 - kappa) & 127)

            def send(r, carry):
                nodes = [face[r, n] for n in range(N)]
                for m in range(N):
                    total = splat[t, m * N] * nodes[0]
                    for n in range(1, N):
                        total = total + splat[t, m * N + n] * nodes[n]
                    dst1[t, 3, r, m] = pltpu.roll(total, shifts[m], 1)
                for h in range(2):
                    for j in range(3):
                        first_hop(t, r, h, j).start()

                @pl.when(side == 2)
                def _():
                    for h in range(2):
                        own_hop(t, r, h).start()

                return carry

            lax.fori_loop(0, N, send, 0)

        @pl.when(t == 0)
        def _():
            for copy in load_rest:
                copy.wait()

            @pl.when(is_mortar)
            def _():
                def body(r, carry):
                    for cc in range(N):
                        total = re[fm, r, cc]
                        for p in range(N):
                            total = total + float(DERIV[p, 0]) ** 2 * jnp.where(
                                parity == 1, co[0, 6 - p, r, cc], co[0, p, r, cc]
                            )
                        diag[r, cc] = total
                    return carry

                lax.fori_loop(0, N, body, 0)

        lax.fori_loop(jnp.where(is_mortar, 1, 0), N, next_slice, 0)
        lax.fori_loop(0, N, ends, 0)

        def pack(a, carry):
            low, high = carry
            for r in range(N):
                here = lane == a * N + r
                low = jnp.where(here, jnp.broadcast_to(ap[a, r, 0][:, 0:1], (8, 128)), low)
                high = jnp.where(here, jnp.broadcast_to(ap[a, r, 6][:, 127:128], (8, 128)), high)
            return low, high

        zero = jnp.zeros((8, 128), jnp.float32)
        low, high = lax.fori_loop(0, N, pack, (zero, zero))
        halo_src[t, 0] = low
        halo_src[t, 1] = high
        low_copy = hop(halo_src.at[t, 0], halo_dst.at[t, 0], halo_send.at[0], halo_recv.at[t % 2, 0], prv, side)
        high_copy = hop(halo_src.at[t, 1], halo_dst.at[t, 1], halo_send.at[1], halo_recv.at[t % 2, 1], nxt, side)
        low_copy.start()
        high_copy.start()

        def first_relay(r, carry):
            @pl.when(is_relay)
            def _():
                for h in range(2):
                    @pl.when(side == 3)
                    def _():
                        landed(dst1.at[t, pl.ds(0, 4), r, nodes_of(h)], recv1.at[t % 2, r, h])

                    @pl.when(side == 1)
                    def _():
                        landed(dst1.at[t, pl.ds(0, 3), r, nodes_of(h)], recv1.at[t % 2, r, h])

                    which = jnp.where(z_first(r, h), 0, 1)
                    for m in range(PIECES[h][0], sum(PIECES[h])):
                        src2[t, r, m] = pick(
                            codes[t, which, m], dst1[t, 3, r, m], [dst1[t, j, r, m] for j in range(3)]
                        )
                    for j in range(3):
                        second_hop(t, r, h, j).start()

            axial(r, (1, 2, 3, 4, 5))
            return carry

        lax.fori_loop(0, N, first_relay, 0)

        side_copy = hop(ap.at[fp], side_dst.at[t], side_send, side_recv.at[t % 2], c, partner)
        side_copy.start()

        def relay(r, carry):
            @pl.when(is_relay)
            def _():
                for h in range(2):
                    landed(dst2.at[t, pl.ds(0, 3), r, nodes_of(h)], recv2.at[t % 2, r, h])
                    which = jnp.where(z_first(r, h), 2, 0)
                    for m in range(PIECES[h][0], sum(PIECES[h])):
                        src3[t, r, m] = pick(
                            codes[t, which, m], src2[t, r, m], [dst2[t, j, r, m] for j in range(3)]
                        )
                    for j in range(2):
                        last_hop(t, r, h, j).start()

            return carry

        lax.fori_loop(0, N, relay, 0)

        low_copy.wait()
        high_copy.wait()

        def advance(a, carry):
            after, before = carry
            for r in range(N):
                for cc in range(N):
                    total = ap[a, r, cc]
                    if r == 6:
                        total = total + jnp.where(row == 7, 0.0, pltpu.roll(ap[a, 0, cc], 7, 0))
                    if r == 0:
                        total = total + jnp.where(row == 0, 0.0, pltpu.roll(ap[a, 6, cc], 1, 0))
                    if cc == 6:
                        other = jnp.broadcast_to(after[:, r:r + 1], (8, 128))
                        total = total + jnp.where(lane == 127, other, pltpu.roll(ap[a, r, 0], 127, 1))
                    if cc == 0:
                        other = jnp.broadcast_to(before[:, r:r + 1], (8, 128))
                        total = total + jnp.where(lane == 0, other, pltpu.roll(ap[a, r, 6], 1, 1))
                    u[a, r, cc] = u[a, r, cc] - sc[a, r, cc] * total
            return pltpu.roll(after, 128 - N, 1), pltpu.roll(before, 128 - N, 1)

        lax.fori_loop(0, N, advance, (halo_dst[t, 0], halo_dst[t, 1]))
        side_copy.wait()

        def add_side(r, carry):
            for cc in range(N):
                u[fp, r, cc] = u[fp, r, cc] - sc[fp, r, cc] * side_dst[t, r, cc]
            return carry

        lax.fori_loop(0, N, add_side, 0)


        @pl.when(is_mortar & (t < STEPS - 1))
        def _():
            in_face(fm)
            first_face()

        @pl.when(is_mortar)
        def _():
            def arrive(r, carry):
                landed(dst3.at[t, pl.ds(0, 2), r], recv3.at[t % 2, r])
                nodes = [
                    jnp.where(codes[t, 3, m] == 0, dst3[t, 0, r, m], dst3[t, 1, r, m])
                    for m in range(N)
                ]
                changes = []
                for n in range(N):
                    total = splat[t, N * N + n * N] * nodes[0]
                    for m in range(1, N):
                        total = total + splat[t, N * N + n * N + m] * nodes[m]
                    change = -(sc[fm, r, n] * total)
                    changes.append(change)
                    delta[r, n] = change
                    u[fm, r, n] = u[fm, r, n] + change

                @pl.when(t < STEPS - 1)
                def _():
                    res = apply_line(changes, [co[2, fm, r, p] for p in range(N)])
                    for n in range(N):
                        face[r, n] = face[r, n] + res[n] + diag[r, n] * changes[n]

                return carry

            lax.fori_loop(0, N, arrive, 0)

            @pl.when(t < STEPS - 1)
            def _():
                for cc in range(N):
                    line = [delta[r, cc] for r in range(N)]
                    res = apply_line(line, [co[1, fm, p, cc] for p in range(N)])
                    for r in range(N):
                        face[r, cc] = face[r, cc] + res[r]

        return carry

    lax.fori_loop(0, STEPS, step, 0)

    every = pl.ds(0, STEPS)

    @pl.when(is_mortar)
    def _():
        sent(dst1.at[every, pl.ds(0, 3)], 0)

    @pl.when(side == 2)
    def _():
        sent(dst1.at[every, 3], 1)

    @pl.when(is_relay)
    def _():
        sent(dst2, 2)
        sent(dst3, 3)


def local(field, coeffs, reaction, step_scale, rotation):
    block = field.shape[1:]
    tile = block[-2:]
    f32 = jnp.float32
    dma = pltpu.SemaphoreType.DMA
    table = jnp.asarray(mortar_constants().reshape(-1))
    hbm_spec = pl.BlockSpec(memory_space=pltpu.HBM)
    smem_spec = pl.BlockSpec(memory_space=pltpu.SMEM)

    def face_buffers(*lead):
        return pltpu.VMEM((*lead, N, N, *tile), f32)

    result = pl.pallas_call(
        kernel,
        out_shape=pltpu.VMEM(block, f32),
        in_specs=[smem_spec, smem_spec, hbm_spec, hbm_spec, hbm_spec, hbm_spec],
        out_specs=pl.BlockSpec(memory_space=pltpu.VMEM),
        scratch_shapes=[
            pltpu.VMEM((3, *block), f32),
            pltpu.VMEM(block, f32),
            pltpu.VMEM(block, f32),
            pltpu.VMEM(block, f32),
            pltpu.VMEM((STEPS, 2 * N * N, *tile), f32),
            pltpu.VMEM((STEPS, 4, N, *tile), jnp.int32),
            face_buffers(),
            face_buffers(),
            face_buffers(),
            pltpu.VMEM((STEPS, 2, *tile), f32),
            pltpu.VMEM((STEPS, 2, *tile), f32),
            face_buffers(STEPS),
            face_buffers(STEPS, 4),
            face_buffers(STEPS),
            face_buffers(STEPS, 3),
            face_buffers(STEPS),
            face_buffers(STEPS, 2),
            dma((7,)),
            dma((2,)),
            dma((2, 2)),
            dma,
            dma((2,)),
            dma((4,)),
            dma((2, N, 2)),
            dma((2, N, 2)),
            dma((2, N)),
        ],
        compiler_params=pltpu.CompilerParams(
            collective_id=0, has_side_effects=True, vmem_limit_bytes=61 * 1024 * 1024
        ),
    )(rotation, table, field[0], coeffs[0], reaction[0], step_scale[0])
    return result[None]


def solution(mesh):
    in_specs = (
        P("side", None, None, None, None, "circ"),
        P("side", None, None, None, None, None, "circ"),
        P("side", None, None, None, None, "circ"),
        P("side", None, None, None, None, "circ"),
        P(),
    )
    out_specs = P("side", None, None, None, None, "circ")
    return jax.shard_map(local, mesh=mesh, in_specs=in_specs, out_specs=out_specs, check_vma=False)
```

```python
import jax
import jax.numpy as jnp
import numpy as np
from jax import lax
from jax.experimental import pallas as pl
from jax.experimental.pallas import tpu as pltpu
from jax.sharding import PartitionSpec as P

SUBSTEPS = 3
STEPS = 4
N = 7
NY = 4
NZ = 4
PIECES = ((0, 4), (4, 3))
MESH = pl.DeviceIdType.MESH


def gll_points():
    return np.array(
        [-1.0, -0.830223896278567, -0.4688487934707142, 0.0,
         0.4688487934707142, 0.830223896278567, 1.0]
    )


def derivative_table():
    points = gll_points()
    weights = np.array(
        [1.0 / np.prod([points[j] - points[k] for k in range(N) if k != j]) for j in range(N)]
    )
    derivative = np.zeros((N, N))
    for i in range(N):
        for j in range(N):
            if i != j:
                derivative[i, j] = weights[j] / weights[i] / (points[i] - points[j])
        derivative[i, i] = -np.sum(derivative[i])
    return derivative


def lagrange_row(location):
    points = gll_points()
    return np.array(
        [np.prod([(location - points[q]) / (points[n] - points[q]) for q in range(N) if q != n])
         for n in range(N)]
    )


def mortar_constants():
    heights = (1.0 + gll_points()) * 0.5
    table = np.zeros((2, SUBSTEPS, 2, N, N))
    for residue in range(SUBSTEPS):
        fraction = residue / SUBSTEPS
        rows = []
        for m in range(N):
            local = heights[m] - fraction
            if heights[m] < fraction:
                local += 1.0
            rows.append(lagrange_row(2.0 * local - 1.0))
        both = np.array(rows)
        table[0, residue, 0] = both
        table[0, residue, 1] = both.T
        table[1, residue, 0] = np.eye(N)
        table[1, residue, 1] = np.eye(N)
    return table.astype(np.float32)


def left_counts():
    heights = (1.0 + gll_points()) * 0.5
    return [int(np.sum(heights < residue / SUBSTEPS)) for residue in range(SUBSTEPS)]


DERIV = derivative_table()
LEFT = left_counts()


def half_line(matrix, v):
    even = [v[q] + v[6 - q] for q in range(3)]
    odd = [v[q] - v[6 - q] for q in range(3)]
    out = [None] * N
    for p in range(3):
        e = float(matrix[p, 3]) * v[3]
        o = None
        for q in range(3):
            e = e + float(0.5 * (matrix[p, q] + matrix[p, 6 - q])) * even[q]
            term = float(0.5 * (matrix[p, q] - matrix[p, 6 - q])) * odd[q]
            o = term if o is None else o + term
        out[p] = o + e
        out[6 - p] = o - e
    out[3] = (
        float(matrix[3, 0]) * odd[0] + float(matrix[3, 1]) * odd[1] + float(matrix[3, 2]) * odd[2]
    )
    return out


def apply_line(v, coeff):
    grad = half_line(DERIV, v)
    return half_line(DERIV.T, [coeff[p] * grad[p] for p in range(N)])


def kernel(
    rot, table, field, coeffs, reaction, scale, u,
    co, re, sc, ap, splat, codes, face, delta, diag,
    halo_src, halo_dst, side_dst,
    dst1, src2, dst2, src3, dst3,
    load_sem, halo_send, halo_recv, side_send, side_recv,
    sends, recv1, recv2, recv3,
):
    c = lax.axis_index("circ")
    side = lax.axis_index("side")
    count = lax.axis_size("circ")
    z_me = c % NZ
    y_me = (c // NZ) % NY
    x_me = c // (NZ * NY)
    parity = side % 2
    is_mortar = (side == 1) | (side == 2)
    is_relay = parity == 1
    is_rotor = side < 2
    partner = side + 1 - 2 * parity
    fp = 6 - 6 * parity
    fm = 6 * parity
    lane = lax.broadcasted_iota(jnp.int32, (8, 128), 1)
    row = lax.broadcasted_iota(jnp.int32, (8, 128), 0)

    def at(xx, yy, zz):
        return (xx * NY + yy) * NZ + zz

    nxt = (c + 1) % count
    prv = (c + count - 1) % count
    z_dev = [at(x_me, y_me, (z_me + j + 1) % NZ) for j in range(3)]
    y_dev = [at(x_me, (y_me + j + 1) % NY, z_me) for j in range(3)]
    x_dev = [at((x_me + j) % 2, y_me, z_me) for j in range(2)]
    first_side = jnp.where(side == 1, 1, 3)
    last_side = jnp.where(side == 1, 2, 1)

    def ordered(i):
        return jnp.where(parity == 1, 6 - i, i)

    rest_of = pl.ds(1 - parity, N - 1)
    in_layer = pl.ds(1, 2)

    def load(i, src, dst):
        return pltpu.make_async_copy(src, dst, load_sem.at[i])

    load_first = [
        load(0, field, u),
        load(1, coeffs.at[in_layer, fm], co.at[in_layer, fm]),
        load(2, reaction.at[fm], re.at[fm]),
    ]
    load_axial = load(3, coeffs.at[0], co.at[0])
    load_rest = [
        load(4, coeffs.at[in_layer, rest_of], co.at[in_layer, rest_of]),
        load(5, reaction.at[rest_of], re.at[rest_of]),
        load(6, scale, sc),
    ]

    barrier = pltpu.get_barrier_semaphore()

    def greet(cc, ss):
        pl.semaphore_signal(
            barrier, inc=1, device_id={"circ": cc, "side": ss}, device_id_type=MESH
        )

    greet(nxt, side)
    greet(prv, side)
    greet(c, partner)

    ring = z_dev + y_dev
    peers = {
        1: [(d, 1) for d in ring] + [(d, 3) for d in x_dev],
        2: [(d, 1) for d in x_dev],
        3: [(d, 2) for d in ring] + [(d, 3) for d in ring],
    }
    targets = {0: 3, 1: 3 + 6 + 2, 2: 3 + 6, 3: 3 + 6 + 2}

    def greet_peers(which):
        @pl.when(side == which)
        def _():
            for d, ss in peers[which]:
                greet(d, ss)

    for which in peers:
        greet_peers(which)

    for copy in load_first + [load_axial] + load_rest:
        copy.start()

    def digits(shift):
        s = shift & 127
        total = ((shift >> 7) + jnp.where(lane < s, 1, 0)) & 31
        dz = total & 3
        dy = (total >> 2) & 3
        late = dy + jnp.where(z_me < dz, 1, 0)
        early = dy + jnp.where(z_me + dz > 3, 1, 0)
        dx = ((total >> 4) + jnp.where(y_me < late, 1, 0)) & 1
        return dz, early & 3, late & 3, dx

    @pl.when(side > 0)
    def _():
        def prepare(t, carry):
            offset = rot[t]
            k = offset // SUBSTEPS
            residue = offset - k * SUBSTEPS
            left = jnp.where(residue == 0, LEFT[0], jnp.where(residue == 1, LEFT[1], LEFT[2]))
            cycle = count * 128
            for m in range(N):
                kappa = k + jnp.where(m < left, 1, 0)
                kappa = jnp.where(kappa >= cycle, kappa - cycle, kappa)
                back = jnp.where(kappa == 0, 0, cycle - kappa)
                dz, early, late, _ = digits(jnp.where(is_rotor, kappa, back))
                codes[t, 0, m] = dz
                codes[t, 1, m] = early
                codes[t, 2, m] = late
                codes[t, 3, m] = digits(jnp.where(is_rotor, back, kappa))[3]
            half = jnp.where(is_rotor, 0, 1)
            first = (half * SUBSTEPS + residue) * 2 * N * N
            for i in range(2 * N * N):
                splat[t, i] = jnp.full((8, 128), table[first + i], jnp.float32)
            return carry

        lax.fori_loop(0, STEPS, prepare, 0)

    def in_face(a):
        for cc in range(N):
            line = [u[a, r, cc] for r in range(N)]
            res = apply_line(line, [co[1, a, p, cc] for p in range(N)])
            for r in range(N):
                ap[a, r, cc] = res[r] + re[a, r, cc] * line[r]
        for r in range(N):
            line = [u[a, r, cc] for cc in range(N)]
            res = apply_line(line, [co[2, a, r, p] for p in range(N)])
            for cc in range(N):
                ap[a, r, cc] = ap[a, r, cc] + res[cc]

    def axial(r, columns):
        for cc in columns:
            line = [u[a, r, cc] for a in range(N)]
            res = apply_line(line, [co[0, p, r, cc] for p in range(N)])
            for a in range(N):
                ap[a, r, cc] = ap[a, r, cc] + res[a]

        @pl.when(is_mortar)
        def _():
            for cc in columns:
                ap[fm, r, cc] = face[r, cc]

    def next_slice(i, carry):
        in_face(ordered(i))
        return carry

    def ends(r, carry):
        axial(r, (0, 6))
        return carry

    edge = [jnp.where(parity == 1, float(DERIV[p, 6]), float(DERIV[p, 0])) for p in range(N)]

    for copy in load_first:
        copy.wait()
    in_face(fm)
    load_axial.wait()

    def first_face():
        def body(r, carry):
            for cc in range(N):
                grad = half_line(DERIV, [u[a, r, cc] for a in range(N)])
                total = ap[fm, r, cc]
                for p in range(N):
                    total = total + edge[p] * (co[0, p, r, cc] * grad[p])
                face[r, cc] = total
            return carry

        lax.fori_loop(0, N, body, 0)

    @pl.when(is_mortar)
    def _():
        first_face()

    def meet(which):
        @pl.when(side == which)
        def _():
            pl.semaphore_wait(barrier, targets[which])

    for which in range(4):
        meet(which)

    def hop(src, dst, send, recv, cc, ss):
        return pltpu.make_async_remote_copy(
            src_ref=src, dst_ref=dst, send_sem=send, recv_sem=recv,
            device_id={"circ": cc, "side": ss}, device_id_type=MESH,
        )

    def nodes_of(h):
        return pl.ds(*PIECES[h])

    def z_first(r, h):
        return r % 2 == h

    def first_hop(t, r, h, j):
        dev = jnp.where(z_first(r, h), z_dev[j], y_dev[j])
        return hop(dst1.at[t, 3, r, nodes_of(h)], dst1.at[t, j, r, nodes_of(h)],
                   sends.at[0], recv1.at[t % 2, r], dev, first_side)

    def own_hop(t, r, h):
        return hop(dst1.at[t, 3, r, nodes_of(h)], dst1.at[t, 3, r, nodes_of(h)],
                   sends.at[1], recv1.at[t % 2, r], c, partner)

    def second_hop(t, r, h, j):
        dev = jnp.where(z_first(r, h), y_dev[j], z_dev[j])
        return hop(src2.at[t, r, nodes_of(h)], dst2.at[t, j, r, nodes_of(h)],
                   sends.at[2], recv2.at[t % 2, r], dev, side)

    def last_hop(t, r, h, j):
        return hop(src3.at[t, r, nodes_of(h)], dst3.at[t, j, r, nodes_of(h)],
                   sends.at[3], recv3.at[t % 2, r], x_dev[j], last_side)

    def landed(ref, sem):
        hop(ref, ref, sends.at[0], sem, c, partner).wait_recv()

    def sent(ref, i):
        hop(ref, ref, sends.at[i], recv3.at[0, 0], c, partner).wait_send()

    def pick(code, own, others):
        low = jnp.where(code == 0, own, others[0])
        high = jnp.where(code == 2, others[1], others[2])
        return jnp.where(code < 2, low, high)

    def step(t, carry):
        @pl.when(is_mortar)
        def _():
            offset = rot[t]
            k = offset // SUBSTEPS
            residue = offset - k * SUBSTEPS
            left = jnp.where(residue == 0, LEFT[0], jnp.where(residue == 1, LEFT[1], LEFT[2]))
            shifts = []
            for m in range(N):
                kappa = k + jnp.where(m < left, 1, 0)
                shifts.append(jnp.where(is_rotor, kappa, 128 * 64 - kappa) & 127)

            def send(r, carry):
                nodes = [face[r, n] for n in range(N)]
                for m in range(N):
                    total = splat[t, m * N] * nodes[0]
                    for n in range(1, N):
                        total = total + splat[t, m * N + n] * nodes[n]
                    dst1[t, 3, r, m] = pltpu.roll(total, shifts[m], 1)
                for h in range(2):
                    for j in (1, 0, 2):
                        first_hop(t, r, h, j).start()

                @pl.when(side == 2)
                def _():
                    for h in range(2):
                        own_hop(t, r, h).start()

                return carry

            lax.fori_loop(0, N, send, 0)

        @pl.when(t == 0)
        def _():
            for copy in load_rest:
                copy.wait()

            @pl.when(is_mortar)
            def _():
                def body(r, carry):
                    for cc in range(N):
                        total = re[fm, r, cc]
                        for p in range(N):
                            total = total + float(DERIV[p, 0]) ** 2 * jnp.where(
                                parity == 1, co[0, 6 - p, r, cc], co[0, p, r, cc]
                            )
                        diag[r, cc] = total
                    return carry

                lax.fori_loop(0, N, body, 0)

        lax.fori_loop(jnp.where(is_mortar, 1, 0), N, next_slice, 0)
        lax.fori_loop(0, N, ends, 0)

        def pack(a, carry):
            low, high = carry
            for r in range(N):
                here = lane == a * N + r
                low = jnp.where(here, jnp.broadcast_to(ap[a, r, 0][:, 0:1], (8, 128)), low)
                high = jnp.where(here, jnp.broadcast_to(ap[a, r, 6][:, 127:128], (8, 128)), high)
            return low, high

        zero = jnp.zeros((8, 128), jnp.float32)
        low, high = lax.fori_loop(0, N, pack, (zero, zero))
        halo_src[t, 0] = low
        halo_src[t, 1] = high
        low_copy = hop(halo_src.at[t, 0], halo_dst.at[t, 0], halo_send.at[0], halo_recv.at[t % 2, 0], prv, side)
        high_copy = hop(halo_src.at[t, 1], halo_dst.at[t, 1], halo_send.at[1], halo_recv.at[t % 2, 1], nxt, side)
        low_copy.start()
        high_copy.start()

        def first_relay(r, carry):
            @pl.when(is_relay)
            def _():
                @pl.when(side == 3)
                def _():
                    landed(dst1.at[t, pl.ds(0, 4), r], recv1.at[t % 2, r])

                @pl.when(side == 1)
                def _():
                    landed(dst1.at[t, pl.ds(0, 3), r], recv1.at[t % 2, r])

                for h in range(2):
                    which = jnp.where(z_first(r, h), 0, 1)
                    for m in range(PIECES[h][0], sum(PIECES[h])):
                        src2[t, r, m] = pick(
                            codes[t, which, m], dst1[t, 3, r, m], [dst1[t, j, r, m] for j in range(3)]
                        )
                    for j in (1, 0, 2):
                        second_hop(t, r, h, j).start()

            axial(r, (1, 2, 3, 4, 5))
            return carry

        lax.fori_loop(0, N, first_relay, 0)

        side_copy = hop(ap.at[fp], side_dst.at[t], side_send, side_recv.at[t % 2], c, partner)
        side_copy.start()

        def relay(r, carry):
            @pl.when(is_relay)
            def _():
                landed(dst2.at[t, pl.ds(0, 3), r], recv2.at[t % 2, r])
                for h in range(2):
                    which = jnp.where(z_first(r, h), 2, 0)
                    for m in range(PIECES[h][0], sum(PIECES[h])):
                        src3[t, r, m] = pick(
                            codes[t, which, m], src2[t, r, m], [dst2[t, j, r, m] for j in range(3)]
                        )
                    for j in range(2):
                        last_hop(t, r, h, j).start()

            return carry

        lax.fori_loop(0, N, relay, 0)

        low_copy.wait()
        high_copy.wait()

        def advance(a, carry):
            after, before = carry
            for r in range(N):
                for cc in range(N):
                    total = ap[a, r, cc]
                    if r == 6:
                        total = total + jnp.where(row == 7, 0.0, pltpu.roll(ap[a, 0, cc], 7, 0))
                    if r == 0:
                        total = total + jnp.where(row == 0, 0.0, pltpu.roll(ap[a, 6, cc], 1, 0))
                    if cc == 6:
                        other = jnp.broadcast_to(after[:, r:r + 1], (8, 128))
                        total = total + jnp.where(lane == 127, other, pltpu.roll(ap[a, r, 0], 127, 1))
                    if cc == 0:
                        other = jnp.broadcast_to(before[:, r:r + 1], (8, 128))
                        total = total + jnp.where(lane == 0, other, pltpu.roll(ap[a, r, 6], 1, 1))
                    u[a, r, cc] = u[a, r, cc] - sc[a, r, cc] * total
            return pltpu.roll(after, 128 - N, 1), pltpu.roll(before, 128 - N, 1)

        lax.fori_loop(0, N, advance, (halo_dst[t, 0], halo_dst[t, 1]))
        side_copy.wait()

        def add_side(r, carry):
            for cc in range(N):
                u[fp, r, cc] = u[fp, r, cc] - sc[fp, r, cc] * side_dst[t, r, cc]
            return carry

        lax.fori_loop(0, N, add_side, 0)


        @pl.when(is_mortar & (t < STEPS - 1))
        def _():
            in_face(fm)
            first_face()

        @pl.when(is_mortar)
        def _():
            def arrive(r, carry):
                landed(dst3.at[t, pl.ds(0, 2), r], recv3.at[t % 2, r])
                nodes = [
                    jnp.where(codes[t, 3, m] == 0, dst3[t, 0, r, m], dst3[t, 1, r, m])
                    for m in range(N)
                ]
                changes = []
                for n in range(N):
                    total = splat[t, N * N + n * N] * nodes[0]
                    for m in range(1, N):
                        total = total + splat[t, N * N + n * N + m] * nodes[m]
                    change = -(sc[fm, r, n] * total)
                    changes.append(change)
                    delta[r, n] = change
                    u[fm, r, n] = u[fm, r, n] + change

                @pl.when(t < STEPS - 1)
                def _():
                    res = apply_line(changes, [co[2, fm, r, p] for p in range(N)])
                    for n in range(N):
                        face[r, n] = face[r, n] + res[n] + diag[r, n] * changes[n]

                return carry

            lax.fori_loop(0, N, arrive, 0)

            @pl.when(t < STEPS - 1)
            def _():
                for cc in range(N):
                    line = [delta[r, cc] for r in range(N)]
                    res = apply_line(line, [co[1, fm, p, cc] for p in range(N)])
                    for r in range(N):
                        face[r, cc] = face[r, cc] + res[r]

        return carry

    lax.fori_loop(0, STEPS, step, 0)

    every = pl.ds(0, STEPS)

    @pl.when(is_mortar)
    def _():
        sent(dst1.at[every, pl.ds(0, 3)], 0)

    @pl.when(side == 2)
    def _():
        sent(dst1.at[every, 3], 1)

    @pl.when(is_relay)
    def _():
        sent(dst2, 2)
        sent(dst3, 3)


def local(field, coeffs, reaction, step_scale, rotation):
    block = field.shape[1:]
    tile = block[-2:]
    f32 = jnp.float32
    dma = pltpu.SemaphoreType.DMA
    table = jnp.asarray(mortar_constants().reshape(-1))
    hbm_spec = pl.BlockSpec(memory_space=pltpu.HBM)
    smem_spec = pl.BlockSpec(memory_space=pltpu.SMEM)

    def face_buffers(*lead):
        return pltpu.VMEM((*lead, N, N, *tile), f32)

    result = pl.pallas_call(
        kernel,
        out_shape=pltpu.VMEM(block, f32),
        in_specs=[smem_spec, smem_spec, hbm_spec, hbm_spec, hbm_spec, hbm_spec],
        out_specs=pl.BlockSpec(memory_space=pltpu.VMEM),
        scratch_shapes=[
            pltpu.VMEM((3, *block), f32),
            pltpu.VMEM(block, f32),
            pltpu.VMEM(block, f32),
            pltpu.VMEM(block, f32),
            pltpu.VMEM((STEPS, 2 * N * N, *tile), f32),
            pltpu.VMEM((STEPS, 4, N, *tile), jnp.int32),
            face_buffers(),
            face_buffers(),
            face_buffers(),
            pltpu.VMEM((STEPS, 2, *tile), f32),
            pltpu.VMEM((STEPS, 2, *tile), f32),
            face_buffers(STEPS),
            face_buffers(STEPS, 4),
            face_buffers(STEPS),
            face_buffers(STEPS, 3),
            face_buffers(STEPS),
            face_buffers(STEPS, 2),
            dma((7,)),
            dma((2,)),
            dma((2, 2)),
            dma,
            dma((2,)),
            dma((4,)),
            dma((2, N)),
            dma((2, N)),
            dma((2, N)),
        ],
        compiler_params=pltpu.CompilerParams(
            collective_id=0, has_side_effects=True, vmem_limit_bytes=61 * 1024 * 1024
        ),
    )(rotation, table, field[0], coeffs[0], reaction[0], step_scale[0])
    return result[None]


def solution(mesh):
    in_specs = (
        P("side", None, None, None, None, "circ"),
        P("side", None, None, None, None, None, "circ"),
        P("side", None, None, None, None, "circ"),
        P("side", None, None, None, None, "circ"),
        P(),
    )
    out_specs = P("side", None, None, None, None, "circ")
    return jax.shard_map(local, mesh=mesh, in_specs=in_specs, out_specs=out_specs, check_vma=False)
```

```python
import jax
import jax.numpy as jnp
import numpy as np
from jax import lax
from jax.experimental import pallas as pl
from jax.experimental.pallas import tpu as pltpu
from jax.sharding import PartitionSpec as P

SUBSTEPS = 3
STEPS = 4
N = 7
NY = 4
NZ = 4
PIECES = ((0, 4), (4, 3))
MESH = pl.DeviceIdType.MESH


def gll_points():
    return np.array(
        [-1.0, -0.830223896278567, -0.4688487934707142, 0.0,
         0.4688487934707142, 0.830223896278567, 1.0]
    )


def derivative_table():
    points = gll_points()
    weights = np.array(
        [1.0 / np.prod([points[j] - points[k] for k in range(N) if k != j]) for j in range(N)]
    )
    derivative = np.zeros((N, N))
    for i in range(N):
        for j in range(N):
            if i != j:
                derivative[i, j] = weights[j] / weights[i] / (points[i] - points[j])
        derivative[i, i] = -np.sum(derivative[i])
    return derivative


def lagrange_row(location):
    points = gll_points()
    return np.array(
        [np.prod([(location - points[q]) / (points[n] - points[q]) for q in range(N) if q != n])
         for n in range(N)]
    )


def mortar_constants():
    heights = (1.0 + gll_points()) * 0.5
    table = np.zeros((2, SUBSTEPS, 2, N, N))
    for residue in range(SUBSTEPS):
        fraction = residue / SUBSTEPS
        rows = []
        for m in range(N):
            local = heights[m] - fraction
            if heights[m] < fraction:
                local += 1.0
            rows.append(lagrange_row(2.0 * local - 1.0))
        both = np.array(rows)
        table[0, residue, 0] = both
        table[0, residue, 1] = both.T
        table[1, residue, 0] = np.eye(N)
        table[1, residue, 1] = np.eye(N)
    return table.astype(np.float32)


def left_counts():
    heights = (1.0 + gll_points()) * 0.5
    return [int(np.sum(heights < residue / SUBSTEPS)) for residue in range(SUBSTEPS)]


DERIV = derivative_table()
LEFT = left_counts()


def half_line(matrix, v):
    even = [v[q] + v[6 - q] for q in range(3)]
    odd = [v[q] - v[6 - q] for q in range(3)]
    out = [None] * N
    for p in range(3):
        e = float(matrix[p, 3]) * v[3]
        o = None
        for q in range(3):
            e = e + float(0.5 * (matrix[p, q] + matrix[p, 6 - q])) * even[q]
            term = float(0.5 * (matrix[p, q] - matrix[p, 6 - q])) * odd[q]
            o = term if o is None else o + term
        out[p] = o + e
        out[6 - p] = o - e
    out[3] = (
        float(matrix[3, 0]) * odd[0] + float(matrix[3, 1]) * odd[1] + float(matrix[3, 2]) * odd[2]
    )
    return out


def apply_line(v, coeff):
    grad = half_line(DERIV, v)
    return half_line(DERIV.T, [coeff[p] * grad[p] for p in range(N)])


def kernel(
    rot_in, table_in, field, coeffs, reaction, scale, u,
    co, re, sc, ap, splat, codes, face, delta, diag,
    halo_src, halo_dst, side_dst,
    dst1, src2, dst2, src3, dst3,
    load_sem, halo_send, halo_recv, side_send, side_recv,
    sends, recv1, recv2, recv3, rot, table,
):
    c = lax.axis_index("circ")
    side = lax.axis_index("side")
    count = lax.axis_size("circ")
    z_me = c % NZ
    y_me = (c // NZ) % NY
    x_me = c // (NZ * NY)
    parity = side % 2
    is_mortar = (side == 1) | (side == 2)
    is_relay = parity == 1
    is_rotor = side < 2
    partner = side + 1 - 2 * parity
    fp = 6 - 6 * parity
    fm = 6 * parity
    lane = lax.broadcasted_iota(jnp.int32, (8, 128), 1)
    row = lax.broadcasted_iota(jnp.int32, (8, 128), 0)

    def at(xx, yy, zz):
        return (xx * NY + yy) * NZ + zz

    nxt = (c + 1) % count
    prv = (c + count - 1) % count
    z_dev = [at(x_me, y_me, (z_me + j + 1) % NZ) for j in range(3)]
    y_dev = [at(x_me, (y_me + j + 1) % NY, z_me) for j in range(3)]
    x_dev = [at((x_me + j) % 2, y_me, z_me) for j in range(2)]
    first_side = jnp.where(side == 1, 1, 3)
    last_side = jnp.where(side == 1, 2, 1)

    def ordered(i):
        return jnp.where(parity == 1, 6 - i, i)

    rest_of = pl.ds(1 - parity, N - 1)
    in_layer = pl.ds(1, 2)

    def load(i, src, dst):
        return pltpu.make_async_copy(src, dst, load_sem.at[i])

    load_first = [
        load(0, field, u),
        load(1, coeffs.at[in_layer, fm], co.at[in_layer, fm]),
        load(2, reaction.at[fm], re.at[fm]),
    ]
    load_axial = load(3, coeffs.at[0], co.at[0])
    load_rest = [
        load(4, coeffs.at[in_layer, rest_of], co.at[in_layer, rest_of]),
        load(5, reaction.at[rest_of], re.at[rest_of]),
        load(6, scale, sc),
    ]

    barrier = pltpu.get_barrier_semaphore()

    def greet(cc, ss):
        pl.semaphore_signal(
            barrier, inc=1, device_id={"circ": cc, "side": ss}, device_id_type=MESH
        )

    greet(nxt, side)
    greet(prv, side)
    greet(c, partner)

    ring = z_dev + y_dev
    peers = {
        1: [(d, 1) for d in ring] + [(d, 3) for d in x_dev],
        2: [(d, 1) for d in x_dev],
        3: [(d, 2) for d in ring] + [(d, 3) for d in ring],
    }
    targets = {0: 3, 1: 3 + 6 + 2, 2: 3 + 6, 3: 3 + 6 + 2}

    def greet_peers(which):
        @pl.when(side == which)
        def _():
            for d, ss in peers[which]:
                greet(d, ss)

    for which in peers:
        greet_peers(which)

    load_small = [load(7, rot_in, rot), load(8, table_in, table)]
    for copy in load_small + load_first + [load_axial] + load_rest:
        copy.start()
    for copy in load_small:
        copy.wait()

    def digits(shift):
        s = shift & 127
        total = ((shift >> 7) + jnp.where(lane < s, 1, 0)) & 31
        dz = total & 3
        dy = (total >> 2) & 3
        late = dy + jnp.where(z_me < dz, 1, 0)
        early = dy + jnp.where(z_me + dz > 3, 1, 0)
        dx = ((total >> 4) + jnp.where(y_me < late, 1, 0)) & 1
        return dz, early & 3, late & 3, dx

    @pl.when(side > 0)
    def _():
        def prepare(t, carry):
            offset = rot[t]
            k = offset // SUBSTEPS
            residue = offset - k * SUBSTEPS
            left = jnp.where(residue == 0, LEFT[0], jnp.where(residue == 1, LEFT[1], LEFT[2]))
            cycle = count * 128
            for m in range(N):
                kappa = k + jnp.where(m < left, 1, 0)
                kappa = jnp.where(kappa >= cycle, kappa - cycle, kappa)
                back = jnp.where(kappa == 0, 0, cycle - kappa)
                dz, early, late, _ = digits(jnp.where(is_rotor, kappa, back))
                codes[t, 0, m] = dz
                codes[t, 1, m] = early
                codes[t, 2, m] = late
                codes[t, 3, m] = digits(jnp.where(is_rotor, back, kappa))[3]
            half = jnp.where(is_rotor, 0, 1)
            first = (half * SUBSTEPS + residue) * 2 * N * N
            for i in range(2 * N * N):
                splat[t, i] = jnp.full((8, 128), table[first + i], jnp.float32)
            return carry

        lax.fori_loop(0, STEPS, prepare, 0)

    def in_face(a):
        for cc in range(N):
            line = [u[a, r, cc] for r in range(N)]
            res = apply_line(line, [co[1, a, p, cc] for p in range(N)])
            for r in range(N):
                ap[a, r, cc] = res[r] + re[a, r, cc] * line[r]
        for r in range(N):
            line = [u[a, r, cc] for cc in range(N)]
            res = apply_line(line, [co[2, a, r, p] for p in range(N)])
            for cc in range(N):
                ap[a, r, cc] = ap[a, r, cc] + res[cc]

    def axial(r, columns):
        for cc in columns:
            line = [u[a, r, cc] for a in range(N)]
            res = apply_line(line, [co[0, p, r, cc] for p in range(N)])
            for a in range(N):
                ap[a, r, cc] = ap[a, r, cc] + res[a]

        @pl.when(is_mortar)
        def _():
            for cc in columns:
                ap[fm, r, cc] = face[r, cc]

    def next_slice(i, carry):
        in_face(ordered(i))
        return carry

    def ends(r, carry):
        axial(r, (0, 6))
        return carry

    edge = [jnp.where(parity == 1, float(DERIV[p, 6]), float(DERIV[p, 0])) for p in range(N)]

    for copy in load_first:
        copy.wait()
    in_face(fm)
    load_axial.wait()

    def first_face():
        def body(r, carry):
            for cc in range(N):
                grad = half_line(DERIV, [u[a, r, cc] for a in range(N)])
                total = ap[fm, r, cc]
                for p in range(N):
                    total = total + edge[p] * (co[0, p, r, cc] * grad[p])
                face[r, cc] = total
            return carry

        lax.fori_loop(0, N, body, 0)

    @pl.when(is_mortar)
    def _():
        first_face()

    def meet(which):
        @pl.when(side == which)
        def _():
            pl.semaphore_wait(barrier, targets[which])

    for which in range(4):
        meet(which)

    def hop(src, dst, send, recv, cc, ss):
        return pltpu.make_async_remote_copy(
            src_ref=src, dst_ref=dst, send_sem=send, recv_sem=recv,
            device_id={"circ": cc, "side": ss}, device_id_type=MESH,
        )

    def nodes_of(h):
        return pl.ds(*PIECES[h])

    def z_first(r, h):
        return r % 2 == h

    def first_hop(t, r, h, j):
        dev = jnp.where(z_first(r, h), z_dev[j], y_dev[j])
        return hop(dst1.at[t, 3, r, nodes_of(h)], dst1.at[t, j, r, nodes_of(h)],
                   sends.at[0], recv1.at[t % 2, r], dev, first_side)

    def own_hop(t, r, h):
        return hop(dst1.at[t, 3, r, nodes_of(h)], dst1.at[t, 3, r, nodes_of(h)],
                   sends.at[1], recv1.at[t % 2, r], c, partner)

    def second_hop(t, r, h, j):
        dev = jnp.where(z_first(r, h), y_dev[j], z_dev[j])
        return hop(src2.at[t, r, nodes_of(h)], dst2.at[t, j, r, nodes_of(h)],
                   sends.at[2], recv2.at[t % 2, r], dev, side)

    def last_hop(t, r, h, j):
        return hop(src3.at[t, r, nodes_of(h)], dst3.at[t, j, r, nodes_of(h)],
                   sends.at[3], recv3.at[t % 2, r], x_dev[j], last_side)

    def landed(ref, sem):
        hop(ref, ref, sends.at[0], sem, c, partner).wait_recv()

    def sent(ref, i):
        hop(ref, ref, sends.at[i], recv3.at[0, 0], c, partner).wait_send()

    def pick(code, own, others):
        low = jnp.where(code == 0, own, others[0])
        high = jnp.where(code == 2, others[1], others[2])
        return jnp.where(code < 2, low, high)

    def step(t, carry):
        @pl.when(is_mortar)
        def _():
            offset = rot[t]
            k = offset // SUBSTEPS
            residue = offset - k * SUBSTEPS
            left = jnp.where(residue == 0, LEFT[0], jnp.where(residue == 1, LEFT[1], LEFT[2]))
            shifts = []
            for m in range(N):
                kappa = k + jnp.where(m < left, 1, 0)
                shifts.append(jnp.where(is_rotor, kappa, 128 * 64 - kappa) & 127)

            def send(r, carry):
                nodes = [face[r, n] for n in range(N)]
                for m in range(N):
                    total = splat[t, m * N] * nodes[0]
                    for n in range(1, N):
                        total = total + splat[t, m * N + n] * nodes[n]
                    dst1[t, 3, r, m] = pltpu.roll(total, shifts[m], 1)
                for h in range(2):
                    for j in (1, 0, 2):
                        first_hop(t, r, h, j).start()

                @pl.when(side == 2)
                def _():
                    for h in range(2):
                        own_hop(t, r, h).start()

                return carry

            lax.fori_loop(0, N, send, 0)

        @pl.when(t == 0)
        def _():
            for copy in load_rest:
                copy.wait()

            @pl.when(is_mortar)
            def _():
                def body(r, carry):
                    for cc in range(N):
                        total = re[fm, r, cc]
                        for p in range(N):
                            total = total + float(DERIV[p, 0]) ** 2 * jnp.where(
                                parity == 1, co[0, 6 - p, r, cc], co[0, p, r, cc]
                            )
                        diag[r, cc] = total
                    return carry

                lax.fori_loop(0, N, body, 0)

        lax.fori_loop(jnp.where(is_mortar, 1, 0), N, next_slice, 0)
        lax.fori_loop(0, N, ends, 0)

        def pack(a, carry):
            low, high = carry
            for r in range(N):
                here = lane == a * N + r
                low = jnp.where(here, jnp.broadcast_to(ap[a, r, 0][:, 0:1], (8, 128)), low)
                high = jnp.where(here, jnp.broadcast_to(ap[a, r, 6][:, 127:128], (8, 128)), high)
            return low, high

        zero = jnp.zeros((8, 128), jnp.float32)
        low, high = lax.fori_loop(0, N, pack, (zero, zero))
        halo_src[t, 0] = low
        halo_src[t, 1] = high
        low_copy = hop(halo_src.at[t, 0], halo_dst.at[t, 0], halo_send.at[0], halo_recv.at[t % 2, 0], prv, side)
        high_copy = hop(halo_src.at[t, 1], halo_dst.at[t, 1], halo_send.at[1], halo_recv.at[t % 2, 1], nxt, side)
        low_copy.start()
        high_copy.start()

        def first_relay(r, carry):
            @pl.when(is_relay)
            def _():
                @pl.when(side == 3)
                def _():
                    landed(dst1.at[t, pl.ds(0, 4), r], recv1.at[t % 2, r])

                @pl.when(side == 1)
                def _():
                    landed(dst1.at[t, pl.ds(0, 3), r], recv1.at[t % 2, r])

                for h in range(2):
                    which = jnp.where(z_first(r, h), 0, 1)
                    for m in range(PIECES[h][0], sum(PIECES[h])):
                        src2[t, r, m] = pick(
                            codes[t, which, m], dst1[t, 3, r, m], [dst1[t, j, r, m] for j in range(3)]
                        )
                    for j in (1, 0, 2):
                        second_hop(t, r, h, j).start()

            axial(r, (1, 2, 3, 4, 5))
            return carry

        lax.fori_loop(0, N, first_relay, 0)

        side_copy = hop(ap.at[fp], side_dst.at[t], side_send, side_recv.at[t % 2], c, partner)
        side_copy.start()

        def relay(r, carry):
            @pl.when(is_relay)
            def _():
                landed(dst2.at[t, pl.ds(0, 3), r], recv2.at[t % 2, r])
                for h in range(2):
                    which = jnp.where(z_first(r, h), 2, 0)
                    for m in range(PIECES[h][0], sum(PIECES[h])):
                        src3[t, r, m] = pick(
                            codes[t, which, m], src2[t, r, m], [dst2[t, j, r, m] for j in range(3)]
                        )
                    for j in range(2):
                        last_hop(t, r, h, j).start()

            return carry

        lax.fori_loop(0, N, relay, 0)

        low_copy.wait()
        high_copy.wait()

        def advance(a, carry):
            after, before = carry
            for r in range(N):
                for cc in range(N):
                    total = ap[a, r, cc]
                    if r == 6:
                        total = total + jnp.where(row == 7, 0.0, pltpu.roll(ap[a, 0, cc], 7, 0))
                    if r == 0:
                        total = total + jnp.where(row == 0, 0.0, pltpu.roll(ap[a, 6, cc], 1, 0))
                    if cc == 6:
                        other = jnp.broadcast_to(after[:, r:r + 1], (8, 128))
                        total = total + jnp.where(lane == 127, other, pltpu.roll(ap[a, r, 0], 127, 1))
                    if cc == 0:
                        other = jnp.broadcast_to(before[:, r:r + 1], (8, 128))
                        total = total + jnp.where(lane == 0, other, pltpu.roll(ap[a, r, 6], 1, 1))
                    u[a, r, cc] = u[a, r, cc] - sc[a, r, cc] * total
            return pltpu.roll(after, 128 - N, 1), pltpu.roll(before, 128 - N, 1)

        lax.fori_loop(0, N, advance, (halo_dst[t, 0], halo_dst[t, 1]))
        side_copy.wait()

        def add_side(r, carry):
            for cc in range(N):
                u[fp, r, cc] = u[fp, r, cc] - sc[fp, r, cc] * side_dst[t, r, cc]
            return carry

        lax.fori_loop(0, N, add_side, 0)


        @pl.when(is_mortar & (t < STEPS - 1))
        def _():
            in_face(fm)
            first_face()

        @pl.when(is_mortar)
        def _():
            def arrive(r, carry):
                landed(dst3.at[t, pl.ds(0, 2), r], recv3.at[t % 2, r])
                nodes = [
                    jnp.where(codes[t, 3, m] == 0, dst3[t, 0, r, m], dst3[t, 1, r, m])
                    for m in range(N)
                ]
                changes = []
                for n in range(N):
                    total = splat[t, N * N + n * N] * nodes[0]
                    for m in range(1, N):
                        total = total + splat[t, N * N + n * N + m] * nodes[m]
                    change = -(sc[fm, r, n] * total)
                    changes.append(change)
                    delta[r, n] = change
                    u[fm, r, n] = u[fm, r, n] + change

                @pl.when(t < STEPS - 1)
                def _():
                    res = apply_line(changes, [co[2, fm, r, p] for p in range(N)])
                    for n in range(N):
                        face[r, n] = face[r, n] + res[n] + diag[r, n] * changes[n]

                return carry

            lax.fori_loop(0, N, arrive, 0)

            @pl.when(t < STEPS - 1)
            def _():
                for cc in range(N):
                    line = [delta[r, cc] for r in range(N)]
                    res = apply_line(line, [co[1, fm, p, cc] for p in range(N)])
                    for r in range(N):
                        face[r, cc] = face[r, cc] + res[r]

        return carry

    lax.fori_loop(0, STEPS, step, 0)

    every = pl.ds(0, STEPS)

    @pl.when(is_mortar)
    def _():
        sent(dst1.at[every, pl.ds(0, 3)], 0)

    @pl.when(side == 2)
    def _():
        sent(dst1.at[every, 3], 1)

    @pl.when(is_relay)
    def _():
        sent(dst2, 2)
        sent(dst3, 3)


def local(field, coeffs, reaction, step_scale, rotation):
    block = field.shape[1:]
    tile = block[-2:]
    f32 = jnp.float32
    dma = pltpu.SemaphoreType.DMA
    table = jnp.asarray(mortar_constants().reshape(-1))
    hbm_spec = pl.BlockSpec(memory_space=pltpu.HBM)

    def face_buffers(*lead):
        return pltpu.VMEM((*lead, N, N, *tile), f32)

    result = pl.pallas_call(
        kernel,
        out_shape=pltpu.VMEM(block, f32),
        in_specs=[hbm_spec, hbm_spec, hbm_spec, hbm_spec, hbm_spec, hbm_spec],
        out_specs=pl.BlockSpec(memory_space=pltpu.VMEM),
        scratch_shapes=[
            pltpu.VMEM((3, *block), f32),
            pltpu.VMEM(block, f32),
            pltpu.VMEM(block, f32),
            pltpu.VMEM(block, f32),
            pltpu.VMEM((STEPS, 2 * N * N, *tile), f32),
            pltpu.VMEM((STEPS, 4, N, *tile), jnp.int32),
            face_buffers(),
            face_buffers(),
            face_buffers(),
            pltpu.VMEM((STEPS, 2, *tile), f32),
            pltpu.VMEM((STEPS, 2, *tile), f32),
            face_buffers(STEPS),
            face_buffers(STEPS, 4),
            face_buffers(STEPS),
            face_buffers(STEPS, 3),
            face_buffers(STEPS),
            face_buffers(STEPS, 2),
            dma((9,)),
            dma((2,)),
            dma((2, 2)),
            dma,
            dma((2,)),
            dma((4,)),
            dma((2, N)),
            dma((2, N)),
            dma((2, N)),
            pltpu.SMEM(rotation.shape, jnp.int32),
            pltpu.SMEM(table.shape, f32),
        ],
        compiler_params=pltpu.CompilerParams(
            collective_id=0, has_side_effects=True, vmem_limit_bytes=61 * 1024 * 1024
        ),
    )(rotation, table, field[0], coeffs[0], reaction[0], step_scale[0])
    return result[None]


def solution(mesh):
    in_specs = (
        P("side", None, None, None, None, "circ"),
        P("side", None, None, None, None, None, "circ"),
        P("side", None, None, None, None, "circ"),
        P("side", None, None, None, None, "circ"),
        P(),
    )
    out_specs = P("side", None, None, None, None, "circ")
    return jax.shard_map(local, mesh=mesh, in_specs=in_specs, out_specs=out_specs, check_vma=False)
```

```python
import jax
import jax.numpy as jnp
import numpy as np
from jax import lax
from jax.experimental import pallas as pl
from jax.experimental.pallas import tpu as pltpu
from jax.sharding import PartitionSpec as P

SUBSTEPS = 3
STEPS = 4
N = 7
NY = 4
NZ = 4
PIECES = ((0, 4), (4, 3))
MESH = pl.DeviceIdType.MESH


def gll_points():
    return np.array(
        [-1.0, -0.830223896278567, -0.4688487934707142, 0.0,
         0.4688487934707142, 0.830223896278567, 1.0]
    )


def derivative_table():
    points = gll_points()
    weights = np.array(
        [1.0 / np.prod([points[j] - points[k] for k in range(N) if k != j]) for j in range(N)]
    )
    derivative = np.zeros((N, N))
    for i in range(N):
        for j in range(N):
            if i != j:
                derivative[i, j] = weights[j] / weights[i] / (points[i] - points[j])
        derivative[i, i] = -np.sum(derivative[i])
    return derivative


def lagrange_row(location):
    points = gll_points()
    return np.array(
        [np.prod([(location - points[q]) / (points[n] - points[q]) for q in range(N) if q != n])
         for n in range(N)]
    )


def mortar_constants():
    heights = (1.0 + gll_points()) * 0.5
    table = np.zeros((2, SUBSTEPS, 2, N, N))
    for residue in range(SUBSTEPS):
        fraction = residue / SUBSTEPS
        rows = []
        for m in range(N):
            local = heights[m] - fraction
            if heights[m] < fraction:
                local += 1.0
            rows.append(lagrange_row(2.0 * local - 1.0))
        both = np.array(rows)
        table[0, residue, 0] = both
        table[0, residue, 1] = both.T
        table[1, residue, 0] = np.eye(N)
        table[1, residue, 1] = np.eye(N)
    return table.astype(np.float32)


def left_counts():
    heights = (1.0 + gll_points()) * 0.5
    return [int(np.sum(heights < residue / SUBSTEPS)) for residue in range(SUBSTEPS)]


DERIV = derivative_table()
LEFT = left_counts()


def half_line(matrix, v):
    even = [v[q] + v[6 - q] for q in range(3)]
    odd = [v[q] - v[6 - q] for q in range(3)]
    out = [None] * N
    for p in range(3):
        e = float(matrix[p, 3]) * v[3]
        o = None
        for q in range(3):
            e = e + float(0.5 * (matrix[p, q] + matrix[p, 6 - q])) * even[q]
            term = float(0.5 * (matrix[p, q] - matrix[p, 6 - q])) * odd[q]
            o = term if o is None else o + term
        out[p] = o + e
        out[6 - p] = o - e
    out[3] = (
        float(matrix[3, 0]) * odd[0] + float(matrix[3, 1]) * odd[1] + float(matrix[3, 2]) * odd[2]
    )
    return out


def apply_line(v, coeff):
    grad = half_line(DERIV, v)
    return half_line(DERIV.T, [coeff[p] * grad[p] for p in range(N)])


def kernel(
    rot_in, table_in, field, coeffs, reaction, scale, u,
    co, re, sc, ap, splat, codes, face, delta, diag,
    halo_src, halo_dst, side_dst,
    dst1, src2, dst2, src3, dst3,
    load_sem, halo_send, halo_recv, side_send, side_recv,
    sends, recv1, recv2, recv3, rot, table,
):
    c = lax.axis_index("circ")
    side = lax.axis_index("side")
    count = lax.axis_size("circ")
    z_me = c % NZ
    y_me = (c // NZ) % NY
    x_me = c // (NZ * NY)
    parity = side % 2
    is_mortar = (side == 1) | (side == 2)
    is_relay = parity == 1
    is_rotor = side < 2
    partner = side + 1 - 2 * parity
    fp = 6 - 6 * parity
    fm = 6 * parity
    lane = lax.broadcasted_iota(jnp.int32, (8, 128), 1)
    row = lax.broadcasted_iota(jnp.int32, (8, 128), 0)

    def at(xx, yy, zz):
        return (xx * NY + yy) * NZ + zz

    nxt = (c + 1) % count
    prv = (c + count - 1) % count
    z_dev = [at(x_me, y_me, (z_me + j + 1) % NZ) for j in range(3)]
    y_dev = [at(x_me, (y_me + j + 1) % NY, z_me) for j in range(3)]
    x_dev = [at((x_me + j) % 2, y_me, z_me) for j in range(2)]
    first_side = jnp.where(side == 1, 1, 3)
    last_side = jnp.where(side == 1, 2, 1)

    def ordered(i):
        return jnp.where(parity == 1, 6 - i, i)

    rest_of = pl.ds(1 - parity, N - 1)
    in_layer = pl.ds(1, 2)

    def load(i, src, dst):
        return pltpu.make_async_copy(src, dst, load_sem.at[i])

    load_first = [
        load(0, field, u),
        load(1, coeffs.at[in_layer, fm], co.at[in_layer, fm]),
        load(2, reaction.at[fm], re.at[fm]),
    ]
    load_axial = load(3, coeffs.at[0], co.at[0])
    load_rest = [
        load(4, coeffs.at[in_layer, rest_of], co.at[in_layer, rest_of]),
        load(5, reaction.at[rest_of], re.at[rest_of]),
        load(6, scale, sc),
    ]

    barrier = pltpu.get_barrier_semaphore()

    def greet(cc, ss):
        pl.semaphore_signal(
            barrier, inc=1, device_id={"circ": cc, "side": ss}, device_id_type=MESH
        )

    greet(nxt, side)
    greet(prv, side)
    greet(c, partner)

    ring = z_dev + y_dev
    peers = {
        1: [(d, 1) for d in ring] + [(d, 3) for d in x_dev],
        2: [(d, 1) for d in x_dev],
        3: [(d, 2) for d in ring] + [(d, 3) for d in ring],
    }
    targets = {0: 3, 1: 3 + 6 + 2, 2: 3 + 6, 3: 3 + 6 + 2}

    def greet_peers(which):
        @pl.when(side == which)
        def _():
            for d, ss in peers[which]:
                greet(d, ss)

    for which in peers:
        greet_peers(which)

    load_small = [load(7, rot_in, rot), load(8, table_in, table)]
    for copy in load_small + load_first + [load_axial] + load_rest:
        copy.start()
    for copy in load_small:
        copy.wait()

    def digits(shift):
        s = shift & 127
        total = ((shift >> 7) + jnp.where(lane < s, 1, 0)) & 31
        dz = total & 3
        dy = (total >> 2) & 3
        late = dy + jnp.where(z_me < dz, 1, 0)
        early = dy + jnp.where(z_me + dz > 3, 1, 0)
        dx = ((total >> 4) + jnp.where(y_me < late, 1, 0)) & 1
        return dz, early & 3, late & 3, dx

    @pl.when(side > 0)
    def _():
        def prepare(t, carry):
            offset = rot[t]
            k = offset // SUBSTEPS
            residue = offset - k * SUBSTEPS
            left = jnp.where(residue == 0, LEFT[0], jnp.where(residue == 1, LEFT[1], LEFT[2]))
            cycle = count * 128
            for m in range(N):
                kappa = k + jnp.where(m < left, 1, 0)
                kappa = jnp.where(kappa >= cycle, kappa - cycle, kappa)
                back = jnp.where(kappa == 0, 0, cycle - kappa)
                dz, early, late, _ = digits(jnp.where(is_rotor, kappa, back))
                codes[t, 0, m] = dz
                codes[t, 1, m] = early
                codes[t, 2, m] = late
                codes[t, 3, m] = digits(jnp.where(is_rotor, back, kappa))[3]
            half = jnp.where(is_rotor, 0, 1)
            first = (half * SUBSTEPS + residue) * 2 * N * N
            for i in range(2 * N * N):
                splat[t, i] = jnp.full((8, 128), table[first + i], jnp.float32)
            return carry

        lax.fori_loop(0, STEPS, prepare, 0)

    def in_face(a):
        for cc in range(N):
            line = [u[a, r, cc] for r in range(N)]
            res = apply_line(line, [co[1, a, p, cc] for p in range(N)])
            for r in range(N):
                ap[a, r, cc] = res[r] + re[a, r, cc] * line[r]
        for r in range(N):
            line = [u[a, r, cc] for cc in range(N)]
            res = apply_line(line, [co[2, a, r, p] for p in range(N)])
            for cc in range(N):
                ap[a, r, cc] = ap[a, r, cc] + res[cc]

    def axial(r, columns):
        for cc in columns:
            line = [u[a, r, cc] for a in range(N)]
            res = apply_line(line, [co[0, p, r, cc] for p in range(N)])
            for a in range(N):
                ap[a, r, cc] = ap[a, r, cc] + res[a]

        @pl.when(is_mortar)
        def _():
            for cc in columns:
                ap[fm, r, cc] = face[r, cc]

    def next_slice(i, carry):
        in_face(ordered(i))
        return carry

    def ends(r, carry):
        axial(r, (0, 6))
        return carry

    edge = [jnp.where(parity == 1, float(DERIV[p, 6]), float(DERIV[p, 0])) for p in range(N)]

    for copy in load_first:
        copy.wait()
    in_face(fm)
    load_axial.wait()

    def first_face():
        def body(r, carry):
            for cc in range(N):
                grad = half_line(DERIV, [u[a, r, cc] for a in range(N)])
                total = ap[fm, r, cc]
                for p in range(N):
                    total = total + edge[p] * (co[0, p, r, cc] * grad[p])
                face[r, cc] = total
            return carry

        lax.fori_loop(0, N, body, 0)

    @pl.when(is_mortar)
    def _():
        first_face()

    def meet(which):
        @pl.when(side == which)
        def _():
            pl.semaphore_wait(barrier, targets[which])

    for which in range(4):
        meet(which)

    def hop(src, dst, send, recv, cc, ss):
        return pltpu.make_async_remote_copy(
            src_ref=src, dst_ref=dst, send_sem=send, recv_sem=recv,
            device_id={"circ": cc, "side": ss}, device_id_type=MESH,
        )

    def nodes_of(h):
        return pl.ds(*PIECES[h])

    def z_first(r, h):
        return r % 2 == h

    def first_hop(t, r, h, j):
        dev = jnp.where(z_first(r, h), z_dev[j], y_dev[j])
        return hop(dst1.at[t, 3, r, nodes_of(h)], dst1.at[t, j, r, nodes_of(h)],
                   sends.at[0], recv1.at[t % 2, r], dev, first_side)

    def own_hop(t, r, h):
        return hop(dst1.at[t, 3, r, nodes_of(h)], dst1.at[t, 3, r, nodes_of(h)],
                   sends.at[1], recv1.at[t % 2, r], c, partner)

    def second_hop(t, r, h, j):
        dev = jnp.where(z_first(r, h), y_dev[j], z_dev[j])
        return hop(src2.at[t, r, nodes_of(h)], dst2.at[t, j, r, nodes_of(h)],
                   sends.at[2], recv2.at[t % 2, r], dev, side)

    def last_hop(t, r, h, j):
        return hop(src3.at[t, r, nodes_of(h)], dst3.at[t, j, r, nodes_of(h)],
                   sends.at[3], recv3.at[t % 2, r // 4], x_dev[j], last_side)

    def landed(ref, sem):
        hop(ref, ref, sends.at[0], sem, c, partner).wait_recv()

    def sent(ref, i):
        hop(ref, ref, sends.at[i], recv3.at[0, 0], c, partner).wait_send()

    def pick(code, own, others):
        low = jnp.where(code == 0, own, others[0])
        high = jnp.where(code == 2, others[1], others[2])
        return jnp.where(code < 2, low, high)

    def step(t, carry):
        @pl.when(is_mortar)
        def _():
            offset = rot[t]
            k = offset // SUBSTEPS
            residue = offset - k * SUBSTEPS
            left = jnp.where(residue == 0, LEFT[0], jnp.where(residue == 1, LEFT[1], LEFT[2]))
            shifts = []
            for m in range(N):
                kappa = k + jnp.where(m < left, 1, 0)
                shifts.append(jnp.where(is_rotor, kappa, 128 * 64 - kappa) & 127)

            def send(r, carry):
                nodes = [face[r, n] for n in range(N)]
                for m in range(N):
                    total = splat[t, m * N] * nodes[0]
                    for n in range(1, N):
                        total = total + splat[t, m * N + n] * nodes[n]
                    dst1[t, 3, r, m] = pltpu.roll(total, shifts[m], 1)
                for h in range(2):
                    for j in (1, 0, 2):
                        first_hop(t, r, h, j).start()

                @pl.when(side == 2)
                def _():
                    for h in range(2):
                        own_hop(t, r, h).start()

                return carry

            lax.fori_loop(0, N, send, 0)

        @pl.when(t == 0)
        def _():
            for copy in load_rest:
                copy.wait()

            @pl.when(is_mortar)
            def _():
                def body(r, carry):
                    for cc in range(N):
                        total = re[fm, r, cc]
                        for p in range(N):
                            total = total + float(DERIV[p, 0]) ** 2 * jnp.where(
                                parity == 1, co[0, 6 - p, r, cc], co[0, p, r, cc]
                            )
                        diag[r, cc] = total
                    return carry

                lax.fori_loop(0, N, body, 0)

        lax.fori_loop(jnp.where(is_mortar, 1, 0), N, next_slice, 0)
        lax.fori_loop(0, N, ends, 0)

        def pack(a, carry):
            low, high = carry
            for r in range(N):
                here = lane == a * N + r
                low = jnp.where(here, jnp.broadcast_to(ap[a, r, 0][:, 0:1], (8, 128)), low)
                high = jnp.where(here, jnp.broadcast_to(ap[a, r, 6][:, 127:128], (8, 128)), high)
            return low, high

        zero = jnp.zeros((8, 128), jnp.float32)
        low, high = lax.fori_loop(0, N, pack, (zero, zero))
        halo_src[t, 0] = low
        halo_src[t, 1] = high
        low_copy = hop(halo_src.at[t, 0], halo_dst.at[t, 0], halo_send.at[0], halo_recv.at[t % 2, 0], prv, side)
        high_copy = hop(halo_src.at[t, 1], halo_dst.at[t, 1], halo_send.at[1], halo_recv.at[t % 2, 1], nxt, side)
        low_copy.start()
        high_copy.start()

        def first_relay(r, carry):
            @pl.when(is_relay)
            def _():
                @pl.when(side == 3)
                def _():
                    landed(dst1.at[t, pl.ds(0, 4), r], recv1.at[t % 2, r])

                @pl.when(side == 1)
                def _():
                    landed(dst1.at[t, pl.ds(0, 3), r], recv1.at[t % 2, r])

                for h in range(2):
                    which = jnp.where(z_first(r, h), 0, 1)
                    for m in range(PIECES[h][0], sum(PIECES[h])):
                        src2[t, r, m] = pick(
                            codes[t, which, m], dst1[t, 3, r, m], [dst1[t, j, r, m] for j in range(3)]
                        )
                    for j in (1, 0, 2):
                        second_hop(t, r, h, j).start()

            axial(r, (1, 2, 3, 4, 5))
            return carry

        lax.fori_loop(0, N, first_relay, 0)

        side_copy = hop(ap.at[fp], side_dst.at[t], side_send, side_recv.at[t % 2], c, partner)
        side_copy.start()

        def relay(r, carry):
            @pl.when(is_relay)
            def _():
                landed(dst2.at[t, pl.ds(0, 3), r], recv2.at[t % 2, r])
                for h in range(2):
                    which = jnp.where(z_first(r, h), 2, 0)
                    for m in range(PIECES[h][0], sum(PIECES[h])):
                        src3[t, r, m] = pick(
                            codes[t, which, m], src2[t, r, m], [dst2[t, j, r, m] for j in range(3)]
                        )
                    for j in range(2):
                        last_hop(t, r, h, j).start()

            return carry

        lax.fori_loop(0, N, relay, 0)

        low_copy.wait()
        high_copy.wait()

        def advance(a, carry):
            after, before = carry
            for r in range(N):
                for cc in range(N):
                    total = ap[a, r, cc]
                    if r == 6:
                        total = total + jnp.where(row == 7, 0.0, pltpu.roll(ap[a, 0, cc], 7, 0))
                    if r == 0:
                        total = total + jnp.where(row == 0, 0.0, pltpu.roll(ap[a, 6, cc], 1, 0))
                    if cc == 6:
                        other = jnp.broadcast_to(after[:, r:r + 1], (8, 128))
                        total = total + jnp.where(lane == 127, other, pltpu.roll(ap[a, r, 0], 127, 1))
                    if cc == 0:
                        other = jnp.broadcast_to(before[:, r:r + 1], (8, 128))
                        total = total + jnp.where(lane == 0, other, pltpu.roll(ap[a, r, 6], 1, 1))
                    u[a, r, cc] = u[a, r, cc] - sc[a, r, cc] * total
            return pltpu.roll(after, 128 - N, 1), pltpu.roll(before, 128 - N, 1)

        lax.fori_loop(0, N, advance, (halo_dst[t, 0], halo_dst[t, 1]))
        side_copy.wait()

        def add_side(r, carry):
            for cc in range(N):
                u[fp, r, cc] = u[fp, r, cc] - sc[fp, r, cc] * side_dst[t, r, cc]
            return carry

        lax.fori_loop(0, N, add_side, 0)


        @pl.when(is_mortar & (t < STEPS - 1))
        def _():
            in_face(fm)
            first_face()

        @pl.when(is_mortar)
        def _():
            def arrive(r, carry):
                nodes = [
                    jnp.where(codes[t, 3, m] == 0, dst3[t, 0, r, m], dst3[t, 1, r, m])
                    for m in range(N)
                ]
                changes = []
                for n in range(N):
                    total = splat[t, N * N + n * N] * nodes[0]
                    for m in range(1, N):
                        total = total + splat[t, N * N + n * N + m] * nodes[m]
                    change = -(sc[fm, r, n] * total)
                    changes.append(change)
                    delta[r, n] = change
                    u[fm, r, n] = u[fm, r, n] + change

                @pl.when(t < STEPS - 1)
                def _():
                    res = apply_line(changes, [co[2, fm, r, p] for p in range(N)])
                    for n in range(N):
                        face[r, n] = face[r, n] + res[n] + diag[r, n] * changes[n]

                return carry

            landed(dst3.at[t, pl.ds(0, 2), pl.ds(0, 4)], recv3.at[t % 2, 0])
            lax.fori_loop(0, 4, arrive, 0)
            landed(dst3.at[t, pl.ds(0, 2), pl.ds(4, 3)], recv3.at[t % 2, 1])
            lax.fori_loop(4, N, arrive, 0)

            @pl.when(t < STEPS - 1)
            def _():
                for cc in range(N):
                    line = [delta[r, cc] for r in range(N)]
                    res = apply_line(line, [co[1, fm, p, cc] for p in range(N)])
                    for r in range(N):
                        face[r, cc] = face[r, cc] + res[r]

        return carry

    lax.fori_loop(0, STEPS, step, 0)

    every = pl.ds(0, STEPS)

    @pl.when(is_mortar)
    def _():
        sent(dst1.at[every, pl.ds(0, 3)], 0)

    @pl.when(side == 2)
    def _():
        sent(dst1.at[every, 3], 1)

    @pl.when(is_relay)
    def _():
        sent(dst2, 2)
        sent(dst3, 3)


def local(field, coeffs, reaction, step_scale, rotation):
    block = field.shape[1:]
    tile = block[-2:]
    f32 = jnp.float32
    dma = pltpu.SemaphoreType.DMA
    table = jnp.asarray(mortar_constants().reshape(-1))
    hbm_spec = pl.BlockSpec(memory_space=pltpu.HBM)

    def face_buffers(*lead):
        return pltpu.VMEM((*lead, N, N, *tile), f32)

    result = pl.pallas_call(
        kernel,
        out_shape=pltpu.VMEM(block, f32),
        in_specs=[hbm_spec, hbm_spec, hbm_spec, hbm_spec, hbm_spec, hbm_spec],
        out_specs=pl.BlockSpec(memory_space=pltpu.VMEM),
        scratch_shapes=[
            pltpu.VMEM((3, *block), f32),
            pltpu.VMEM(block, f32),
            pltpu.VMEM(block, f32),
            pltpu.VMEM(block, f32),
            pltpu.VMEM((STEPS, 2 * N * N, *tile), f32),
            pltpu.VMEM((STEPS, 4, N, *tile), jnp.int32),
            face_buffers(),
            face_buffers(),
            face_buffers(),
            pltpu.VMEM((STEPS, 2, *tile), f32),
            pltpu.VMEM((STEPS, 2, *tile), f32),
            face_buffers(STEPS),
            face_buffers(STEPS, 4),
            face_buffers(STEPS),
            face_buffers(STEPS, 3),
            face_buffers(STEPS),
            face_buffers(STEPS, 2),
            dma((9,)),
            dma((2,)),
            dma((2, 2)),
            dma,
            dma((2,)),
            dma((4,)),
            dma((2, N)),
            dma((2, N)),
            dma((2, 2)),
            pltpu.SMEM(rotation.shape, jnp.int32),
            pltpu.SMEM(table.shape, f32),
        ],
        compiler_params=pltpu.CompilerParams(
            collective_id=0, has_side_effects=True, vmem_limit_bytes=61 * 1024 * 1024
        ),
    )(rotation, table, field[0], coeffs[0], reaction[0], step_scale[0])
    return result[None]


def solution(mesh):
    in_specs = (
        P("side", None, None, None, None, "circ"),
        P("side", None, None, None, None, None, "circ"),
        P("side", None, None, None, None, "circ"),
        P("side", None, None, None, None, "circ"),
        P(),
    )
    out_specs = P("side", None, None, None, None, "circ")
    return jax.shard_map(local, mesh=mesh, in_specs=in_specs, out_specs=out_specs, check_vma=False)
```
